256 devices in a mesh: gx: 8 (over z), gy: 8 (over y, core), gz: 4 (over x).
Axes of the slice: x: 4, y: 4, z: 8, core: 2. Of those that a mesh axis runs over, the one named last changes fastest.
Arguments:
- positions: float32 [3, 16, 16, 32, 128], P(None, 'gx', 'gy', 'gz'), may hold values from 0 to 1
- shield: float32 [16, 16, 32, 128], P('gx', 'gy', 'gz'), may hold values from 0.3 to 1
- width: float32 [16, 16, 32, 128], P('gx', 'gy', 'gz'), may hold values from 0.5 to 2
- hardness: float32 [16, 16, 32, 128], P('gx', 'gy', 'gz'), may hold values from 0.5 to 2
- softness: float32 [16, 16, 32, 128], P('gx', 'gy', 'gz'), may hold values from 0.5 to 2
- coupling: float32 [16, 16, 32, 128], P('gx', 'gy', 'gz'), may hold values from -0.45 to 0.45
- pair_bits: int32 [16, 16, 32], P('gx', 'gy', 'gz'), may hold values from 8192 to 134217727, as said below
- right_side: float32 [4, 16, 16, 32, 128], P(None, 'gx', 'gy', 'gz'), may hold values from -7 to 7
Outputs:
- solution: float32 [4, 16, 16, 32, 128], P(None, 'gx', 'gy', 'gz')
- residual: float32 [4, 16, 16, 32, 128], P(None, 'gx', 'gy', 'gz')
The draws below stay inside these ranges and needn't reach their ends.
Inputs may be any that keep to these rules, and one draw needn't show every extreme that they name: `pair_bits`: bit k of a tile's word stands for the offset with code k as in the reference program; bit 13 is always 1, bits 27 and up are 0, a bit is 0 where the offset leaves the grid, and the lists are symmetric: bit k of tile t equals bit 26 - k of the tile at t plus that offset.
All inputs are finite; a program needn't handle non-finite values.
Results may differ from the reference program's by a relative error of at most 0.0018.
Values sent between devices are 32-bit elements; how exact they have to be, the bound alone decides.
A program may use at most 128 MiB of HBM per device.

```python
import math
import jax
import jax.numpy as jnp
from jax import lax

TILE = 128
ITERS = 3
NTX = 16
NTY = 16
NTZ = 32


def draw_pair_bits(key, part):
    forward_bits = jax.random.randint(key, (NTX, NTY, NTZ, 13), 0, 2).astype(jnp.int32)
    padded_bits = jnp.pad(forward_bits, ((1, 1), (1, 1), (1, 1), (0, 0)))
    index_first = lax.broadcasted_iota(jnp.int32, (NTX, NTY, NTZ), 0)
    index_second = lax.broadcasted_iota(jnp.int32, (NTX, NTY, NTZ), 1)
    index_third = lax.broadcasted_iota(jnp.int32, (NTX, NTY, NTZ), 2)
    packed = jnp.full((NTX, NTY, NTZ), 1 << 13, jnp.int32)
    for offset_code in range(27):
        shift_first = offset_code // 9 - 1
        shift_second = offset_code // 3 % 3 - 1
        shift_third = offset_code % 3 - 1
        if offset_code > 13:
            inside = (index_first + shift_first >= 0) & (index_first + shift_first < NTX)
            inside = inside & (index_second + shift_second >= 0) & (index_second + shift_second < NTY)
            inside = inside & (index_third + shift_third >= 0) & (index_third + shift_third < NTZ)
            chosen = jnp.where(inside, forward_bits[:, :, :, offset_code - 14], 0)
            packed = packed + chosen * (1 << offset_code)
        elif offset_code < 13:
            chosen = padded_bits[1 + shift_first:1 + shift_first + NTX, 1 + shift_second:1 + shift_second + NTY, 1 + shift_third:1 + shift_third + NTZ, 12 - offset_code]
            packed = packed + chosen * (1 << offset_code)
    return packed


def draw_right_side(key, part):
    rough_key = jax.random.fold_in(key, 11)
    sign_key = jax.random.fold_in(key, 12)
    wave_key = jax.random.fold_in(key, 13)
    phase_key = jax.random.fold_in(key, 14)
    shape = (4, NTX, NTY, NTZ, TILE)
    rough = jnp.clip(jax.random.normal(rough_key, shape, jnp.float32), -4.0, 4.0)
    signs = jnp.where(jax.random.bernoulli(sign_key, 0.5, (4,)), 1.0, -1.0).astype(jnp.float32)
    waves = jax.random.randint(wave_key, (4, 3), 1, 3).astype(jnp.float32)
    phases = jax.random.uniform(phase_key, (4,), jnp.float32, -math.pi, math.pi)
    coord_first = (lax.broadcasted_iota(jnp.float32, (NTX, NTY, NTZ), 0) + 0.5) / NTX
    coord_second = (lax.broadcasted_iota(jnp.float32, (NTX, NTY, NTZ), 1) + 0.5) / NTY
    coord_third = (lax.broadcasted_iota(jnp.float32, (NTX, NTY, NTZ), 2) + 0.5) / NTZ
    phase_field = waves[:, 0, None, None, None] * coord_first[None] + waves[:, 1, None, None, None] * coord_second[None] + waves[:, 2, None, None, None] * coord_third[None]
    phase_field = 2.0 * math.pi * phase_field + phases[:, None, None, None]
    smooth = signs[:, None, None, None] * (1.0 + 0.5 * jnp.cos(phase_field))
    return (rough + smooth[..., None]).astype(jnp.float32)


def level_of(own_key, dims, pieces, low, top_value):
    def one(position, parts):
        steps = jax.random.uniform(jax.random.fold_in(jax.random.fold_in(own_key, 6), position), (parts,), jnp.float32, low / len(pieces), top_value / len(pieces))
        return jnp.repeat(jnp.exp(steps), dims[position] // parts).reshape((-1,) + (1,) * (len(dims) - position - 1))

    factor_of = one(*pieces[0])
    for cut in pieces[1:]:
        factor_of = factor_of * one(*cut)
    return factor_of


def setup_inputs(seed: int = 0) -> dict:
    key_of = jax.random.split(jax.random.key(seed), 9)
    positions = jnp.clip(1.0 * jax.random.uniform(key_of[0], (3, NTX, NTY, NTZ, TILE), jnp.float32) ** level_of(key_of[0], (3, NTX, NTY, NTZ, TILE), ((1, 8), (2, 8), (3, 4)), -0.2, 0.2), 0.0, 1.0)
    shield = jnp.clip(jnp.exp(math.log(1.0) - 1.2039728 * jax.random.uniform(key_of[1], (NTX, NTY, NTZ, TILE), jnp.float32) ** level_of(key_of[1], (NTX, NTY, NTZ, TILE), ((0, 8), (1, 8), (2, 4)), -0.2, 0.2)), 0.3, 1.0)
    width = jnp.clip(jnp.exp(math.log(2.0) - 1.3862944 * jax.random.uniform(key_of[2], (NTX, NTY, NTZ, TILE), jnp.float32) ** level_of(key_of[2], (NTX, NTY, NTZ, TILE), ((0, 8), (1, 8), (2, 4)), -0.2, 0.2)), 0.5, 2.0)
    hardness = jnp.clip(jnp.exp(math.log(2.0) - 1.3862944 * jax.random.uniform(key_of[3], (NTX, NTY, NTZ, TILE), jnp.float32) ** level_of(key_of[3], (NTX, NTY, NTZ, TILE), ((0, 8), (1, 8), (2, 4)), -0.2, 0.2)), 0.5, 2.0)
    softness = jnp.clip(jnp.exp(math.log(2.0) - 1.3862944 * jax.random.uniform(key_of[4], (NTX, NTY, NTZ, TILE), jnp.float32) ** level_of(key_of[4], (NTX, NTY, NTZ, TILE), ((0, 8), (1, 8), (2, 4)), -0.2, 0.2)), 0.5, 2.0)
    coupling = jnp.clip(jax.random.uniform(key_of[5], (NTX, NTY, NTZ, TILE), jnp.float32, -0.45, 0.45) * level_of(key_of[5], (NTX, NTY, NTZ, TILE), ((0, 8), (1, 8), (2, 4)), -0.4, 0.0), -0.45, 0.45)
    pair_bits = draw_pair_bits(jax.random.fold_in(key_of[8], 71), 0)
    right_side = draw_right_side(jax.random.fold_in(key_of[8], 71), 0)
    return dict(positions=positions, shield=shield, width=width, hardness=hardness, softness=softness, coupling=coupling, pair_bits=pair_bits, right_side=right_side)


coulomb_scale = 0.002
response_scale = 0.003

def index_tuple(values):
    return tuple((jnp.asarray(value).astype(jnp.int32) for value in values))

def pair_terms(own_params, partner, offset_code, own_bits):
    shift_first = (offset_code // 9 - 1).astype(jnp.float32)
    shift_second = (offset_code // 3 % 3 - 1).astype(jnp.float32)
    shift_third = (offset_code % 3 - 1).astype(jnp.float32)

    def separation(column, shift):
        return shift + (partner[column][:, None, :] - own_params[column][:, :, None])
    first = separation(0, shift_first)
    second = separation(1, shift_second)
    third = separation(2, shift_third)
    distance = first * first + second * second + third * third
    coulomb = coulomb_scale * lax.rsqrt(distance + own_params[3][:, :, None] * partner[3][:, None, :])
    response = response_scale * jnp.exp(-distance / (own_params[4][:, :, None] + partner[4][:, None, :]))
    listed = jnp.right_shift(own_bits, offset_code) & 1 > 0
    tile_size = own_params.shape[2]
    diagonal_mask = lax.broadcasted_iota(jnp.int32, (tile_size, tile_size), 0) == lax.broadcasted_iota(jnp.int32, (tile_size, tile_size), 1)
    kept = listed[:, None, None] & jnp.logical_not(diagonal_mask[None] & (offset_code == 13))
    empty_pair = jnp.zeros_like(distance)
    return (jnp.where(kept, coulomb, empty_pair).astype(jnp.bfloat16), jnp.where(kept, response, empty_pair).astype(jnp.bfloat16))

def inner(vector, other_vector):
    return lax.optimization_barrier(jnp.sum((vector * other_vector).reshape(2, 2, -1), axis=(0, 2)))

def widen(scalars):
    return jnp.concatenate([scalars, scalars]).reshape(4, 1, 1, 1, 1)

def reference(positions, shield, width, hardness, softness, coupling, pair_bits, right_side):
    tiles_x, tiles_y, tiles_z, tile_size = hardness.shape
    params = jnp.concatenate([positions, shield[None], width[None]], axis=0)
    params_pad = jnp.pad(params, ((0, 0), (1, 1), (1, 1), (1, 1), (0, 0)))
    plane = tiles_y * tiles_z

    def operate(vector):
        vector_pad = jnp.pad(vector, ((0, 0), (1, 1), (1, 1), (1, 1), (0, 0)))

        def slab_terms(slab_index):
            slab_index = slab_index.astype(jnp.int32)
            own_params = lax.dynamic_slice(params_pad, index_tuple((0, slab_index + 1, 1, 1, 0)), (5, 1, tiles_y, tiles_z, tile_size)).reshape(5, plane, tile_size)
            own_bits = lax.dynamic_slice(pair_bits, index_tuple((slab_index, 0, 0)), (1, tiles_y, tiles_z)).reshape(plane)

            def visit(offset_code, carry):
                row_coulomb, row_response, pair_charge, pair_potential = carry
                offset_code = offset_code.astype(jnp.int32)
                start = index_tuple((0, slab_index + offset_code // 9, offset_code // 3 % 3, offset_code % 3, 0))
                partner = lax.dynamic_slice(params_pad, start, (5, 1, tiles_y, tiles_z, tile_size)).reshape(5, plane, tile_size)
                neighbour = lax.dynamic_slice(vector_pad, start, (4, 1, tiles_y, tiles_z, tile_size)).reshape(4, plane, tile_size)
                coulomb, response = pair_terms(own_params, partner, offset_code, own_bits)
                coulomb = coulomb.astype(jnp.float32)
                response = response.astype(jnp.float32)
                row_coulomb = row_coulomb + lax.optimization_barrier(jnp.sum(coulomb, axis=2))
                row_response = row_response + lax.optimization_barrier(jnp.sum(response, axis=2))
                pair_charge = pair_charge + jnp.einsum('tij,ftj->fti', coulomb, neighbour[:2], precision=lax.Precision.HIGHEST)
                pair_potential = pair_potential + jnp.einsum('tij,ftj->fti', response, neighbour[2:], precision=lax.Precision.HIGHEST)
                return (row_coulomb, row_response, pair_charge, pair_potential)
            flat_zeros = jnp.zeros((plane, tile_size), jnp.float32)
            pair_zeros = jnp.zeros((2, plane, tile_size), jnp.float32)
            return lax.fori_loop(0, 27, visit, (flat_zeros, flat_zeros, pair_zeros, pair_zeros))
        row_coulomb, row_response, pair_charge, pair_potential = lax.map(slab_terms, jnp.arange(tiles_x, dtype=jnp.int32))
        grid = (tiles_x, tiles_y, tiles_z, tile_size)
        row_coulomb = row_coulomb.reshape(grid)
        row_response = row_response.reshape(grid)
        pair_charge = pair_charge.transpose(1, 0, 2, 3).reshape((2,) + grid)
        pair_potential = pair_potential.transpose(1, 0, 2, 3).reshape((2,) + grid)
        image_charge = (hardness + row_coulomb) * vector[:2] + pair_charge + coupling * vector[2:]
        image_potential = (softness + row_response) * vector[2:] - pair_potential + coupling * vector[:2]
        return jnp.concatenate([image_charge, image_potential], axis=0)
    solution = jnp.zeros_like(right_side)
    remainder = right_side
    direction = right_side
    norm_now = inner(remainder, remainder)
    for iteration in range(ITERS):
        applied = operate(direction)
        step_size = norm_now / inner(direction, applied)
        solution = solution + widen(step_size) * direction
        remainder = remainder - widen(step_size) * applied
        norm_next = inner(remainder, remainder)
        direction = remainder + widen(norm_next / norm_now) * direction
        norm_now = norm_next
    residual = right_side - operate(solution)
    return (solution, residual)
```

```python
import itertools

import jax
import jax.numpy as jnp
from jax import lax
from jax.experimental import pallas as pl
from jax.experimental.pallas import tpu as pltpu
from jax.sharding import PartitionSpec as P

MESH = pl.DeviceIdType.MESH
AXES = ("gx", "gy", "gz")
BF = jnp.bfloat16
F32 = jnp.float32
SHIFT = 4.0
LOG2E = 1.4426950408889634
COULOMB_GAIN = 250000.0
RESPONSE_SCALE = 0.003
GROUP = 8
WIDE = 16
DIRECTIONS = [d for d in itertools.product((-1, 0, 1), repeat=3) if d != (0, 0, 0)]
VMEM_SPEC = pl.BlockSpec(memory_space=pltpu.VMEM)
SMEM_SPEC = pl.BlockSpec(memory_space=pltpu.SMEM)


def own_range(step, size):
    return pl.ds(0, size) if step == 0 else pl.ds(size - 1 if step > 0 else 0, 1)


def ghost_range(step, size):
    return pl.ds(1, size) if step == 0 else pl.ds(0 if step > 0 else size + 1, 1)


def neighbour(direction):
    exists = None
    place = []
    for axis, step in zip(AXES, direction):
        at = lax.axis_index(axis) + step
        place.append(at)
        if step:
            inside = at >= 0 if step < 0 else at < lax.axis_size(axis)
            exists = inside if exists is None else exists & inside
    return tuple(place), exists


def greet():
    barrier = pltpu.get_barrier_semaphore()
    count = jnp.int32(0)
    for direction in DIRECTIONS:
        place, exists = neighbour(direction)

        @pl.when(exists)
        def _():
            pl.semaphore_signal(barrier, inc=1, device_id=place, device_id_type=MESH)

        count = count + exists.astype(jnp.int32)
    return barrier, count


def exchange(pairs, send_sem, recv_sem):
    def copies(index, direction, place):
        made = []
        for number, (own, ext) in enumerate(pairs):
            size = own.shape[:3]
            source = own.at[tuple(own_range(s, n) for s, n in zip(direction, size))]
            target = ext.at[tuple(ghost_range(s, n) for s, n in zip(direction, size))]
            made.append(
                pltpu.make_async_remote_copy(
                    source,
                    target,
                    send_sem.at[number, index],
                    recv_sem.at[number, index],
                    device_id=place,
                    device_id_type=MESH,
                )
            )
        return made

    for index, direction in enumerate(DIRECTIONS):
        place, exists = neighbour(direction)

        @pl.when(exists)
        def _():
            for copy in copies(index, direction, place):
                copy.start()

    for index, direction in enumerate(DIRECTIONS):
        place, exists = neighbour(direction)
        source, incoming = neighbour(tuple(-s for s in direction))

        @pl.when(incoming)
        def _():
            for copy in copies(index, direction, place):
                copy.wait_recv()

        @pl.when(exists)
        def _():
            for copy in copies(index, direction, place):
                copy.wait_send()


def first_halo(pos, shield, width, rhs, param_ext, field_ext, param_own, field_own, send_sem, recv_sem):
    param_ext[...] = jnp.zeros_like(param_ext)
    field_ext[...] = jnp.zeros_like(field_ext)
    barrier, count = greet()
    nx, ny, nz = shield.shape[:3]
    for x in range(nx):
        for y in range(ny):
            columns = [pos[0, x, y], pos[1, x, y], pos[2, x, y], shield[x, y], width[x, y]]
            fields = [rhs[f, x, y] for f in range(4)]
            for z in range(nz):
                for f in range(5):
                    row = columns[f][z : z + 1]
                    param_own[x, y, z, f : f + 1, :] = row
                    param_ext[x + 1, y + 1, z + 1, f : f + 1, :] = row
                param_own[x, y, z, 5:8, :] = jnp.zeros((3, 128), F32)
                for f in range(4):
                    row = fields[f][z : z + 1]
                    field_own[x, y, z, f : f + 1, :] = row
                    field_ext[x + 1, y + 1, z + 1, f : f + 1, :] = row
    pl.semaphore_wait(barrier, count)
    exchange(((param_own, param_ext), (field_own, field_ext)), send_sem, recv_sem)


def next_halo(own, ext, send_sem, recv_sem):
    ext[...] = jnp.zeros_like(ext)
    barrier, count = greet()
    ext[1:-1, 1:-1, 1:-1] = own[...]
    pl.semaphore_wait(barrier, count)
    exchange(((own, ext),), send_sem, recv_sem)


def split3(value):
    first = value.astype(BF)
    rest = value - first.astype(F32)
    second = rest.astype(BF)
    third = (rest - second.astype(F32)).astype(BF)
    return first.astype(F32), second.astype(F32), third.astype(F32)


def rows_of(pieces):
    row = lax.broadcasted_iota(jnp.int32, (8, 128), 0)
    value = jnp.zeros((8, 128), F32)
    for index, piece in pieces:
        value = jnp.where(row == index, piece, value)
    return value


def centred(param, ex, ey, ez, half):
    row = lax.broadcasted_iota(jnp.int32, (8, 128), 0)
    offset = jnp.where(row == 0, ex, jnp.where(row == 1, ey, ez)).astype(F32) - jnp.where(
        row == 0, half[0], jnp.where(row == 1, half[1], half[2])
    )
    place = param + offset
    square = jnp.sum(jnp.where(row < 3, place * place, 0.0), axis=0, keepdims=True)
    return row, place, jnp.broadcast_to(square, (8, 128))


def partner_features(param, ex, ey, ez, half):
    row, place, square = centred(param, ex, ey, ez, half)
    value = jnp.where(row < 3, place, jnp.where(row == 3, param, 0.0))
    value = jnp.where(row == 4, square, jnp.where(row == 5, 1.0, value))
    one, two, three = split3(value)
    return jnp.concatenate([one, two, one, two, three, one], axis=0)


def own_features(param, ex, ey, ez, half):
    row, place, square = centred(param, ex, ey, ez, half)
    sides = []
    for gain, shielded in ((-LOG2E, 0.0), (COULOMB_GAIN, COULOMB_GAIN)):
        value = jnp.where(row < 3, (-2.0 * gain) * place, jnp.where(row == 3, shielded * param, 0.0))
        value = jnp.where(row == 4, gain, jnp.where(row == 5, gain * square, value))
        one, two, three = split3(value)
        sides.append(jnp.concatenate([one, one, two, two, one, three], axis=0))
    return jnp.concatenate(sides, axis=1)


def split_fields(ext, halves, tiles):
    ones = jnp.ones((8, 128), F32)

    def step(index, carry):
        for sub in range(8):
            e = index * 8 + sub
            value = ext[e]
            high = value.astype(BF).astype(F32)
            low = value - high
            halves[e] = jnp.concatenate([high, low, ones], axis=0).astype(BF)
        return carry

    lax.fori_loop(0, tiles // 8, step, 0)


def apply_pairs(groups, entries, halves, store, acc):
    acc[...] = jnp.zeros_like(acc)

    def step(index, carry):
        for sub in range(WIDE):
            slot = index * WIDE + sub
            code = entries[slot]
            e = code & 255
            t = lax.shift_right_logical(code, 16)
            both = jnp.concatenate([store[slot, 0], store[slot, 1]], axis=1)
            out = jnp.dot(halves[e], both, preferred_element_type=F32)
            acc[t] = acc[t] + out
        return carry

    lax.fori_loop(0, groups, step, 0)


def diagonal_image(t, out, diagonal, coupling, vector):
    row = lax.broadcasted_iota(jnp.int32, (4, 128), 0)
    summed = out[0:4] + out[4:8]
    pair = jnp.where(row < 2, summed[:, :128], -summed[:, 128:])
    value = vector[t]
    swapped = jnp.concatenate([value[2:4], value[0:2]], axis=0)
    return diagonal * value + pair + coupling[t // 8, pl.ds(t % 8, 1), :] * swapped


def build(
    bits, param, field, own, hardness, softness, coupling, blank, store, entries, count, diagonal, image, send,
    features, mine, halves, acc
):
    ex_size, ey_size, ez_size = 4, 4, 10
    half = (2.0, 2.0, 5.0)
    tiles = ex_size * ey_size * ez_size
    owned = 32

    def features_step(index, carry):
        for sub in range(4):
            e = index * 4 + sub
            ex = e // (ey_size * ez_size)
            ey = (e // ez_size) % ey_size
            ez = e % ez_size
            rows = partner_features(param[e], ex, ey, ez, half)
            features[e, :, 0:48] = rows.T.astype(BF)
        return carry

    lax.fori_loop(0, tiles // 4, features_step, 0)

    def own_step(index, carry):
        for sub in range(2):
            t = index * 2 + sub
            ex = t // 16 + 1
            ey = (t // 8) % 2 + 1
            ez = t % 8 + 1
            e = (ex * ey_size + ey) * ez_size + ez
            mine[t] = own_features(param[e], ex, ey, ez, half).astype(BF)
            entries[t] = e + 256 * t + 65536 * t
        return carry

    lax.fori_loop(0, owned // 2, own_step, 0)
    split_fields(field, halves, tiles)

    def list_step(t, at):
        ex = t // 16 + 1
        ey = (t // 8) % 2 + 1
        ez = t % 8 + 1
        e = (ex * ey_size + ey) * ez_size + ez
        word = bits[t]
        for code in range(27):
            if code == 13:
                continue
            shift = ((code // 9 - 1) * ey_size + (code // 3 % 3 - 1)) * ez_size + code % 3 - 1
            entries[at] = (e + shift) + 256 * t + 65536 * t
            at = at + (lax.shift_right_logical(word, code) & 1)
        return at

    total = lax.fori_loop(0, owned, list_step, jnp.int32(owned))
    middle = (ey_size + 1) * ez_size + 1
    for sub in range(WIDE):
        entries[total + sub] = middle + 65536 * owned
    count[0] = total

    def pair(slot, masked):
        code = entries[slot]
        e = code & 255
        t = lax.shift_right_logical(code, 8) & 255
        both = jnp.dot(features[e, :, 0:48], mine[t], preferred_element_type=F32)
        width_row = param[e, 4:5, :]
        partner_width = jnp.broadcast_to(width_row, (128, 128)).T
        ex = t // 16 + 1
        ey = (t // 8) % 2 + 1
        ez = t % 8 + 1
        here = (ex * ey_size + ey) * ez_size + ez
        widths = partner_width + param[here, 4:5, :]
        coulomb = lax.rsqrt(both[:, 128:])
        response = RESPONSE_SCALE * jnp.exp2(both[:, :128] / widths)
        if masked:
            same = lax.broadcasted_iota(jnp.int32, (128, 128), 0) == lax.broadcasted_iota(
                jnp.int32, (128, 128), 1
            )
            coulomb = jnp.where(same, 0.0, coulomb)
            response = jnp.where(same, 0.0, response)
        store[slot, 0] = coulomb.astype(BF)
        store[slot, 1] = response.astype(BF)

    def self_step(index, carry):
        for sub in range(4):
            pair(index * 4 + sub, True)
        return carry

    lax.fori_loop(0, owned // 4, self_step, 0)

    def pair_step(index, carry):
        for sub in range(GROUP):
            pair(owned + index * GROUP + sub, False)
        return carry

    lax.fori_loop(0, (total - owned + GROUP - 1) // GROUP, pair_step, 0)
    apply_pairs((total + WIDE - 1) // WIDE, entries, halves, store, acc)

    row = lax.broadcasted_iota(jnp.int32, (4, 128), 0)

    def finish(t, carry):
        out = acc[t]
        a, b = t // 8, pl.ds(t % 8, 1)
        top = hardness[a, b, :] + out[8:9, :128]
        low = softness[a, b, :] + out[8:9, 128:]
        diag = jnp.where(row < 2, top, low)
        diagonal[t] = diag
        value = diagonal_image(t, out, diag, coupling, own)
        image[t] = value
        send[t] = value - SHIFT * own[t]
        return carry

    lax.fori_loop(0, owned, finish, 0)


def again(field, own, coupling, store, entries, count, diagonal, image, send, passed, halves, acc):
    owned = 32
    split_fields(field, halves, field.shape[0])
    apply_pairs((count[0] + WIDE - 1) // WIDE, entries, halves, store, acc)

    def finish(t, carry):
        value = diagonal_image(t, acc[t], diagonal[t], coupling, own)
        image[t] = value
        send[t] = value - SHIFT * own[t]
        return carry

    lax.fori_loop(0, owned, finish, 0)


def combine(u0, u1, u2, w0, w1, w2, solution, residual, part, stage, send_sem, recv_sem):
    basis = (u0, u1, u2)
    images = (w0, w1, w2)
    sizes = [lax.axis_size(axis) for axis in AXES]
    places = [lax.axis_index(axis) for axis in AXES]
    barrier = pltpu.get_barrier_semaphore()
    for which, size in enumerate(sizes):
        for step in range(1, size):
            peer = list(places)
            peer[which] = lax.rem(places[which] + step, size)
            pl.semaphore_signal(barrier, inc=1, device_id=tuple(peer), device_id_type=MESH)

    wanted = [(u0, u0), (u0, u1), (u0, u2), (u0, w0), (u0, w1), (u0, w2), (u1, w1), (u1, w2), (u2, w2)]
    sums = []
    for left, right in wanted:
        both = jnp.sum(left[...] * right[...], axis=0)
        sums.append(both[0:2] + both[2:4])
    lane = lax.broadcasted_iota(jnp.int32, (8, 128), 1)
    packed = jnp.zeros((8, 128), F32)
    for block in range(3):
        rows = sums[4 * block : 4 * block + 4]
        rows = rows + [jnp.zeros((2, 128), F32)] * (4 - len(rows))
        folded = jnp.concatenate(rows, axis=0)
        folded = folded + pltpu.roll(folded, 64, 1)
        folded = folded + pltpu.roll(folded, 32, 1)
        packed = jnp.where((lane >= 32 * block) & (lane < 32 * block + 32), folded, packed)
    part[0] = packed
    pl.semaphore_wait(barrier, sum(size - 1 for size in sizes))

    for turn, which in enumerate((2, 1, 0)):
        size = sizes[which]
        made = []
        for step in range(1, size):
            peer = list(places)
            peer[which] = lax.rem(places[which] + step, size)
            copy = pltpu.make_async_remote_copy(
                part.at[turn],
                stage.at[turn, step - 1],
                send_sem.at[turn, step - 1],
                recv_sem.at[turn, step - 1],
                device_id=tuple(peer),
                device_id_type=MESH,
            )
            copy.start()
            made.append(copy)
        mine = part[turn]
        for copy in made:
            copy.wait_recv()
        received = [mine] + [stage[turn, step - 1] for step in range(1, size)]
        total = jnp.zeros((8, 128), F32)
        for place in range(size):
            term = jnp.zeros((8, 128), F32)
            for step in range(size):
                term = jnp.where(lax.rem(places[which] - step + size, size) == place, received[step], term)
            total = total + term
        for copy in made:
            copy.wait_send()
        part[turn + 1] = total

    total = part[3]
    gram = {}
    values = []
    for block in range(3):
        inside = (lane >= 32 * block) & (lane < 32 * block + 32)
        values.append(jnp.sum(jnp.where(inside, total, 0.0), axis=1, keepdims=True))
    value = []
    for index in range(9):
        two = values[index // 4][2 * (index % 4) : 2 * (index % 4) + 2]
        value.append(jnp.concatenate([two, two], axis=0))
    m0, m1, m2, g00, g01, g02, g11, g12, g22 = value
    f1 = g01 / g00
    f2 = g02 / g00
    h11 = g11 - f1 * g01
    h12 = g12 - f1 * g02
    h22 = g22 - f2 * g02
    n1 = m1 - f1 * m0
    n2 = m2 - f2 * m0
    f3 = h12 / h11
    k22 = h22 - f3 * h12
    k2 = n2 - f3 * n1
    c2 = k2 / k22
    c1 = (n1 - h12 * c2) / h11
    c0 = (m0 - g01 * c1 - g02 * c2) / g00
    c0, c1, c2 = (jnp.broadcast_to(c, (4, 128))[None] for c in (c0, c1, c2))
    answer = c0 * u0[...] + c1 * u1[...] + c2 * u2[...]
    left = u0[...] - (c0 * w0[...] + c1 * w1[...] + c2 * w2[...])
    for t in range(32):
        for f in range(4):
            solution[f, t // 8, t % 8 : t % 8 + 1, :] = answer[t, f : f + 1]
            residual[f, t // 8, t % 8 : t % 8 + 1, :] = left[t, f : f + 1]


def on_device(positions, shield, width, hardness, softness, coupling, pair_bits, right_side):
    nx, ny, nz, lanes = hardness.shape
    owned = nx * ny * nz
    ext = (nx + 2, ny + 2, nz + 2)
    tiles = ext[0] * ext[1] * ext[2]
    slots = owned * 27

    def kept(value):
        return pltpu.with_memory_space_constraint(value, pltpu.VMEM)

    def limits(size, **more):
        return pltpu.CompilerParams(vmem_limit_bytes=size, **more)

    param_ext, field_ext, field_own = pl.pallas_call(
        lambda pos, sh, wi, rhs, pe, fe, fo, po, ss, rs: first_halo(pos, sh, wi, rhs, pe, fe, po, fo, ss, rs),
        out_shape=(
            pltpu.VMEM(ext + (8, lanes), F32),
            pltpu.VMEM(ext + (4, lanes), F32),
            pltpu.VMEM((nx, ny, nz, 4, lanes), F32),
        ),
        in_specs=[VMEM_SPEC] * 4,
        out_specs=(VMEM_SPEC,) * 3,
        scratch_shapes=[
            pltpu.VMEM((nx, ny, nz, 8, lanes), F32),
            pltpu.SemaphoreType.DMA((2, 26)),
            pltpu.SemaphoreType.DMA((2, 26)),
        ],
        compiler_params=limits(4 << 20, collective_id=0, has_side_effects=True),
        name="first_halo",
    )(positions, shield, width, right_side)

    hard, soft, link = (a.reshape(owned // 8, 8, lanes) for a in (hardness, softness, coupling))
    own0 = field_own.reshape(owned, 4, lanes)
    vector = jax.ShapeDtypeStruct((owned, 4, lanes), F32)
    blank = pl.pallas_call(
        lambda ref: None,
        out_shape=pltpu.VMEM((slots, 2, lanes, lanes), BF),
        out_specs=VMEM_SPEC,
        compiler_params=limits(1 << 20),
        name="reserve",
    )()
    store, entries, count, diagonal, image0, own1 = pl.pallas_call(
        build,
        out_shape=(
            pltpu.VMEM((slots, 2, lanes, lanes), BF),
            jax.ShapeDtypeStruct((slots + 32,), jnp.int32),
            jax.ShapeDtypeStruct((1,), jnp.int32),
            jax.ShapeDtypeStruct((owned, 4, lanes), F32),
            jax.ShapeDtypeStruct((owned, 4, lanes), F32),
            jax.ShapeDtypeStruct((owned, 4, lanes), F32),
        ),
        in_specs=[SMEM_SPEC] + [VMEM_SPEC] * 7,
        input_output_aliases={7: 0},
        out_specs=(VMEM_SPEC, SMEM_SPEC, SMEM_SPEC, VMEM_SPEC, VMEM_SPEC, VMEM_SPEC),
        scratch_shapes=[
            pltpu.VMEM((tiles, lanes, lanes), BF),
            pltpu.VMEM((owned, 48, 2 * lanes), BF),
            pltpu.VMEM((tiles, 16, lanes), BF),
            pltpu.VMEM((owned + 1, 16, 2 * lanes), F32),
        ],
        compiler_params=limits(8 << 20),
        name="build",
    )(
        pair_bits.reshape(owned),
        kept(param_ext.reshape(tiles, 8, lanes)),
        kept(field_ext.reshape(tiles, 4, lanes)),
        own0,
        hard,
        soft,
        link,
        kept(blank),
    )

    def halo(own, number):
        return pl.pallas_call(
            next_halo,
            out_shape=jax.ShapeDtypeStruct(ext + (4, lanes), F32),
            in_specs=[VMEM_SPEC],
            out_specs=VMEM_SPEC,
            scratch_shapes=[pltpu.SemaphoreType.DMA((1, 26)), pltpu.SemaphoreType.DMA((1, 26))],
            compiler_params=limits(2 << 20, collective_id=number, has_side_effects=True),
            name="halo",
        )(own.reshape(nx, ny, nz, 4, lanes))

    def operate(own, store, number):
        field = halo(own, number)
        return pl.pallas_call(
            again,
            out_shape=(
                jax.ShapeDtypeStruct((owned, 4, lanes), F32),
                jax.ShapeDtypeStruct((owned, 4, lanes), F32),
                pltpu.VMEM(store.shape, BF),
            ),
            in_specs=[VMEM_SPEC] * 4 + [SMEM_SPEC] * 2 + [VMEM_SPEC],
            out_specs=(VMEM_SPEC,) * 3,
            input_output_aliases={3: 2},
            scratch_shapes=[
                pltpu.VMEM((tiles, 16, lanes), BF),
                pltpu.VMEM((owned + 1, 16, 2 * lanes), F32),
            ],
            compiler_params=limits(4 << 20),
            name="apply",
        )(field.reshape(tiles, 4, lanes), own, link, kept(store), entries, count, diagonal)

    image1, own2, store = operate(own1, store, 1)
    image2, _, _ = operate(own2, store, 2)
    sizes = [lax.axis_size(axis) for axis in AXES]
    most = max(sizes) - 1
    shape = jax.ShapeDtypeStruct((4, owned // 8, 8, lanes), F32)
    answer, left = pl.pallas_call(
        combine,
        out_shape=(shape, shape),
        in_specs=[VMEM_SPEC] * 6,
        out_specs=(VMEM_SPEC, VMEM_SPEC),
        scratch_shapes=[
            pltpu.VMEM((4, 8, lanes), F32),
            pltpu.VMEM((3, most, 8, lanes), F32),
            pltpu.SemaphoreType.DMA((3, most)),
            pltpu.SemaphoreType.DMA((3, most)),
        ],
        compiler_params=limits(4 << 20, collective_id=3, has_side_effects=True),
        name="combine",
    )(*(own0, own1, own2, image0, image1, image2))
    out = (4, nx, ny, nz, lanes)
    return answer.reshape(out), left.reshape(out)


def solution(mesh):
    tile = P("gx", "gy", "gz", None)
    field = P(None, "gx", "gy", "gz", None)
    return jax.shard_map(
        on_device,
        mesh=mesh,
        in_specs=(field, tile, tile, tile, tile, tile, P("gx", "gy", "gz"), field),
        out_specs=(field, field),
        check_vma=False,
    )
```

```python
import itertools

import jax
import jax.numpy as jnp
from jax import lax
from jax.experimental import pallas as pl
from jax.experimental.pallas import tpu as pltpu
from jax.sharding import PartitionSpec as P

MESH = pl.DeviceIdType.MESH
AXES = ("gx", "gy", "gz")
BF = jnp.bfloat16
F32 = jnp.float32
SHIFT = 4.0
LOG2E = 1.4426950408889634
COULOMB_GAIN = 250000.0
RESPONSE_SCALE = 0.003
GROUP = 32
WIDE = 32
DIRECTIONS = [d for d in itertools.product((-1, 0, 1), repeat=3) if d != (0, 0, 0)]
VMEM_SPEC = pl.BlockSpec(memory_space=pltpu.VMEM)
SMEM_SPEC = pl.BlockSpec(memory_space=pltpu.SMEM)


def own_range(step, size):
    return pl.ds(0, size) if step == 0 else pl.ds(size - 1 if step > 0 else 0, 1)


def ghost_range(step, size):
    return pl.ds(1, size) if step == 0 else pl.ds(0 if step > 0 else size + 1, 1)


def neighbour(direction):
    exists = None
    place = []
    for axis, step in zip(AXES, direction):
        at = lax.axis_index(axis) + step
        place.append(at)
        if step:
            inside = at >= 0 if step < 0 else at < lax.axis_size(axis)
            exists = inside if exists is None else exists & inside
    return tuple(place), exists


def greet():
    barrier = pltpu.get_barrier_semaphore()
    count = jnp.int32(0)
    for direction in DIRECTIONS:
        place, exists = neighbour(direction)

        @pl.when(exists)
        def _():
            pl.semaphore_signal(barrier, inc=1, device_id=place, device_id_type=MESH)

        count = count + exists.astype(jnp.int32)
    return barrier, count


def exchange(pairs, send_sem, recv_sem):
    def copies(index, direction, place):
        made = []
        for number, (own, ext) in enumerate(pairs):
            size = own.shape[:3]
            source = own.at[tuple(own_range(s, n) for s, n in zip(direction, size))]
            target = ext.at[tuple(ghost_range(s, n) for s, n in zip(direction, size))]
            made.append(
                pltpu.make_async_remote_copy(
                    source,
                    target,
                    send_sem.at[number, index],
                    recv_sem.at[number, index],
                    device_id=place,
                    device_id_type=MESH,
                )
            )
        return made

    for index, direction in enumerate(DIRECTIONS):
        place, exists = neighbour(direction)

        @pl.when(exists)
        def _():
            for copy in copies(index, direction, place):
                copy.start()

    for index, direction in enumerate(DIRECTIONS):
        place, exists = neighbour(direction)
        source, incoming = neighbour(tuple(-s for s in direction))

        @pl.when(incoming)
        def _():
            for copy in copies(index, direction, place):
                copy.wait_recv()

        @pl.when(exists)
        def _():
            for copy in copies(index, direction, place):
                copy.wait_send()


def first_halo(pos_in, shield_in, width_in, rhs_in, param_ext, field_ext, field_own, *scratch):
    param_own, last_own, pos, shield, width, rhs, load_sem, send_sem, recv_sem = scratch
    loads = [
        pltpu.make_async_copy(source, target, load_sem.at[index])
        for index, (source, target) in enumerate(
            ((pos_in, pos), (shield_in, shield), (width_in, width), (rhs_in, rhs))
        )
    ]
    for load in loads:
        load.start()
    param_ext[...] = jnp.zeros_like(param_ext)
    field_ext[...] = jnp.zeros_like(field_ext)
    barrier, count = greet()
    for load in loads:
        load.wait()
    nx, ny, nz = param_own.shape[:3]
    for x in range(nx):
        for y in range(ny):
            columns = [pos[0, x, y], pos[1, x, y], pos[2, x, y], shield[x, y], width[x, y]]
            columns = columns + [rhs[f, x, y] for f in range(4)]
            for z in range(nz):
                for f in range(9):
                    row = columns[f][z : z + 1]
                    if f < 8:
                        param_own[x, y, z, f : f + 1, :] = row
                        param_ext[x + 1, y + 1, z + 1, f : f + 1, :] = row
                    else:
                        last_own[x, y, z] = row
                        field_ext[x + 1, y + 1, z + 1] = row
                    if f > 4:
                        field_own[x, y, z, f - 5 : f - 4, :] = row
    pl.semaphore_wait(barrier, count)
    exchange(((param_own, param_ext), (last_own, field_ext)), send_sem, recv_sem)


def next_halo(own, ext, send_sem, recv_sem):
    ext[...] = jnp.zeros_like(ext)
    barrier, count = greet()
    ext[1:-1, 1:-1, 1:-1] = own[...]
    pl.semaphore_wait(barrier, count)
    exchange(((own, ext),), send_sem, recv_sem)


def split3(value):
    first = value.astype(BF)
    rest = value - first.astype(F32)
    second = rest.astype(BF)
    third = (rest - second.astype(F32)).astype(BF)
    return first.astype(F32), second.astype(F32), third.astype(F32)


def rows_of(pieces):
    row = lax.broadcasted_iota(jnp.int32, (8, 128), 0)
    value = jnp.zeros((8, 128), F32)
    for index, piece in pieces:
        value = jnp.where(row == index, piece, value)
    return value


def centred(param, ex, ey, ez, half):
    row = lax.broadcasted_iota(jnp.int32, (8, 128), 0)
    offset = jnp.where(row == 0, ex, jnp.where(row == 1, ey, ez)).astype(F32) - jnp.where(
        row == 0, half[0], jnp.where(row == 1, half[1], half[2])
    )
    place = param + offset
    square = jnp.sum(jnp.where(row < 3, place * place, 0.0), axis=0, keepdims=True)
    return row, place, jnp.broadcast_to(square, (8, 128))


def partner_features(param, ex, ey, ez, half):
    row, place, square = centred(param, ex, ey, ez, half)
    value = jnp.where(row < 3, place, jnp.where(row == 3, param, 0.0))
    value = jnp.where(row == 4, square, jnp.where(row == 5, 1.0, value))
    one, two, three = split3(value)
    return jnp.concatenate([one, two, one, two, three, one], axis=0)


def own_features(param, ex, ey, ez, half):
    row, place, square = centred(param, ex, ey, ez, half)
    sides = []
    for gain, shielded in ((-LOG2E, 0.0), (COULOMB_GAIN, COULOMB_GAIN)):
        value = jnp.where(row < 3, (-2.0 * gain) * place, jnp.where(row == 3, shielded * param, 0.0))
        value = jnp.where(row == 4, gain, jnp.where(row == 5, gain * square, value))
        one, two, three = split3(value)
        sides.append(jnp.concatenate([one, one, two, two, one, three], axis=0))
    return jnp.concatenate(sides, axis=1)


def split_fields(load, halves, tiles):
    ones = jnp.ones((8, 128), F32)

    def step(index, carry):
        values = [load(index * 16 + sub) for sub in range(16)]
        parts = []
        for value in values:
            high = value.astype(BF).astype(F32)
            parts.append(jnp.concatenate([high, value - high, ones], axis=0).astype(BF))
        for sub in range(16):
            halves[index * 16 + sub] = parts[sub]
        return carry

    lax.fori_loop(0, tiles // 16, step, 0)


def apply_group(base, size, entries, halves, window, acc):
    rows = acc.shape[1]
    for sub in range(size):
        code = entries[base + sub]
        e = code & 255
        t = lax.shift_right_logical(code, 16)
        both = jnp.concatenate([window[sub, 0], window[sub, 1]], axis=1)
        out = jnp.dot(halves[e], both, preferred_element_type=F32)
        acc[t] = acc[t] + out[:rows]


def image_rows(out, diagonal, link, value):
    row = lax.broadcasted_iota(jnp.int32, (4, 128), 0)
    summed = out[0:4] + out[4:8]
    pair = jnp.where(row < 2, summed[:, :128], -summed[:, 128:])
    swapped = jnp.concatenate([value[2:4], value[0:2]], axis=0)
    return diagonal * value + pair + link * swapped


def finish_all(owned, make):
    def step(index, carry):
        results = [make(index, sub) for sub in range(8)]
        for sub, (targets, values) in enumerate(results):
            for target, value in zip(targets, values):
                target[index * 8 + sub] = value
        return carry

    lax.fori_loop(0, owned // 8, step, 0)


def build(
    bits, param, field, own, hardness, softness, coupling, blank, store, entries, count, diagonal, image, send,
    features, mine, halves, acc
):
    ey_size, ez_size = 4, 10
    half = (2.0, 2.0, 5.0)
    tiles = 160
    owned = 32

    def place_of(t):
        return ((t // 16 + 1) * ey_size + t // 8 % 2 + 1) * ez_size + t % 8 + 1

    def features_step(index, at):
        ex = lax.shift_right_logical(index, 2)
        ey = index & 3
        loaded = [param[index * ez_size + ez] for ez in range(ez_size)]
        made = [partner_features(loaded[ez], ex, ey, ez, half).T.astype(BF) for ez in range(ez_size)]
        for ez in range(ez_size):
            features[index * ez_size + ez, :, 0:48] = made[ez]
        for sub in range(2):
            t = index * 2 + sub
            x = lax.shift_right_logical(t, 4)
            y = lax.shift_right_logical(t, 3) & 1
            z = t & 7
            word = bits[x, y, z]
            own_code = ((x + 1) * ey_size + y + 1) * ez_size + z + 1 + 65792 * t
            entries[t] = own_code
            for code in range(27):
                if code == 13:
                    continue
                shift = ((code // 9 - 1) * ey_size + (code // 3 % 3 - 1)) * ez_size + code % 3 - 1
                entries[at] = own_code + shift
                at = at + (lax.shift_right_logical(word, code) & 1)
        return at

    total = lax.fori_loop(0, 16, features_step, jnp.int32(owned))
    middle = (ey_size + 1) * ez_size + 1
    for sub in range(WIDE):
        entries[total + sub] = middle + 65536 * owned
    count[0] = total

    def own_step(index, carry):
        ex = lax.shift_right_logical(index, 1) + 1
        ey = (index & 1) + 1
        first = (ex * ey_size + ey) * ez_size + 1
        made = [own_features(param[first + z], ex, ey, z + 1, half).astype(BF) for z in range(8)]
        for z in range(8):
            mine[index * 8 + z] = made[z]
        return carry

    lax.fori_loop(0, owned // 8, own_step, 0)
    split_fields(lambda e: jnp.concatenate([param[e, 5:8, :], field[e]], axis=0), halves, tiles)
    acc[...] = jnp.zeros_like(acc)

    def pair(slot, window, sub, masked):
        code = entries[slot]
        e = code & 255
        t = lax.shift_right_logical(code, 8) & 255
        both = jnp.dot(features[e, :, 0:48], mine[t], preferred_element_type=F32)
        partner_width = jnp.broadcast_to(param[e, 4:5, :], (128, 128)).T
        widths = partner_width + param[place_of(t), 4:5, :]
        coulomb = lax.rsqrt(both[:, 128:])
        response = RESPONSE_SCALE * jnp.exp2(both[:, :128] / widths)
        if masked:
            same = lax.broadcasted_iota(jnp.int32, (128, 128), 0) == lax.broadcasted_iota(
                jnp.int32, (128, 128), 1
            )
            coulomb = jnp.where(same, 0.0, coulomb)
            response = jnp.where(same, 0.0, response)
        window[sub, 0] = coulomb.astype(BF)
        window[sub, 1] = response.astype(BF)

    def self_step(index, carry):
        window = store.at[pl.ds(index * 8, 8)]
        for sub in range(8):
            pair(index * 8 + sub, window, sub, True)
        return carry

    lax.fori_loop(0, owned // 8, self_step, 0)
    apply_group(0, owned - GROUP, entries, halves, store, acc)

    def pair_step(index, carry):
        base = owned + index * GROUP
        window = store.at[pl.ds(base - GROUP, 2 * GROUP)]
        apply_group(base - GROUP, GROUP, entries, halves, window, acc)
        for sub in range(GROUP):
            pair(base + sub, window, GROUP + sub, False)
        return carry

    groups = (total - owned + GROUP - 1) // GROUP
    lax.fori_loop(0, groups, pair_step, 0)
    last = owned + (groups - 1) * GROUP
    apply_group(last, GROUP, entries, halves, store.at[pl.ds(last, GROUP)], acc)
    row = lax.broadcasted_iota(jnp.int32, (4, 128), 0)

    def make(index, sub):
        out = acc[index * 8 + sub]
        value = own[index * 8 + sub]
        top = hardness[index, sub : sub + 1, :] + out[8:9, :128]
        low = softness[index, sub : sub + 1, :] + out[8:9, 128:]
        diag = jnp.where(row < 2, top, low)
        made = image_rows(out, diag, coupling[index, sub : sub + 1, :], value)
        return (diagonal, image, send), (diag, made, made - SHIFT * value)

    finish_all(owned, make)


def again(field, own, coupling, store, entries, count, diagonal, image, send, passed, halves, acc):
    owned = 32
    split_fields(lambda e: field[e], halves, field.shape[0])
    acc[...] = jnp.zeros_like(acc)

    def step(index, carry):
        apply_group(index * WIDE, WIDE, entries, halves, store.at[pl.ds(index * WIDE, WIDE)], acc)
        return carry

    lax.fori_loop(0, (count[0] + WIDE - 1) // WIDE, step, 0)

    def make(index, sub):
        value = own[index * 8 + sub]
        diag = diagonal[index * 8 + sub]
        made = image_rows(acc[index * 8 + sub], diag, coupling[index, sub : sub + 1, :], value)
        return (image, send), (made, made - SHIFT * value)

    finish_all(owned, make)


def combine(u0, u1, u2, w0, w1, w2, solution, residual, part, plane, line, send_sem, recv_sem):
    sizes = [lax.axis_size(axis) for axis in AXES]
    gx, gy, gz = (lax.axis_index(axis) for axis in AXES)
    across = []
    for a in range(sizes[1]):
        for b in range(sizes[2]):
            if a or b:
                across.append((gx, lax.rem(gy + a, sizes[1]), lax.rem(gz + b, sizes[2])))
    along = [(lax.rem(gx + a, sizes[0]), gy, gz) for a in range(1, sizes[0])]
    barrier = pltpu.get_barrier_semaphore()
    for peer in across + along:
        pl.semaphore_signal(barrier, inc=1, device_id=peer, device_id_type=MESH)

    wanted = [(u0, u0), (u0, u1), (u0, u2), (u0, w0), (u0, w1), (u0, w2), (u1, w1), (u1, w2), (u2, w2)]
    sums = []
    for left, right in wanted:
        both = jnp.sum(left[...] * right[...], axis=0)
        sums.append(both[0:2] + both[2:4])
    stacked = jnp.concatenate(sums + [jnp.zeros((128 - 18, 128), F32)], axis=0)
    part[0] = jnp.sum(stacked.T, axis=0, keepdims=True)
    pl.semaphore_wait(barrier, len(across) + len(along))

    def gather(turn, peers, here, stage, width):
        made = []
        for index, peer in enumerate(peers):
            copy = pltpu.make_async_remote_copy(
                part.at[turn],
                stage.at[here],
                send_sem.at[turn, index],
                recv_sem.at[turn, index],
                device_id=peer,
                device_id_type=MESH,
            )
            copy.start()
            made.append(copy)
        stage[here] = part[turn]
        for copy in made:
            copy.wait_recv()
        total = jnp.sum(stage[...], axis=0)
        for copy in made:
            copy.wait_send()
        return total

    part[1] = gather(0, across, gy * sizes[2] + gz, plane, len(across) + 1)
    total = gather(1, along, gx, line, len(along) + 1)
    m0, m1, m2, g00, g01, g02, g11, g12, g22 = (total[:, 2 * k : 2 * k + 2] for k in range(9))
    f1 = g01 / g00
    f2 = g02 / g00
    h11 = g11 - f1 * g01
    h12 = g12 - f1 * g02
    h22 = g22 - f2 * g02
    n1 = m1 - f1 * m0
    n2 = m2 - f2 * m0
    f3 = h12 / h11
    k22 = h22 - f3 * h12
    k2 = n2 - f3 * n1
    c2 = k2 / k22
    c1 = (n1 - h12 * c2) / h11
    c0 = (m0 - g01 * c1 - g02 * c2) / g00

    def spread(c):
        pair = [jnp.broadcast_to(c[:, r : r + 1], (1, 128)) for r in range(2)]
        return jnp.concatenate(pair + pair, axis=0)[None]

    c0, c1, c2 = (spread(c) for c in (c0, c1, c2))
    answer = c0 * u0[...] + c1 * u1[...] + c2 * u2[...]
    left = u0[...] - (c0 * w0[...] + c1 * w1[...] + c2 * w2[...])
    for t in range(32):
        for f in range(4):
            solution[f, t // 8, t % 8 : t % 8 + 1, :] = answer[t, f : f + 1]
            residual[f, t // 8, t % 8 : t % 8 + 1, :] = left[t, f : f + 1]


def on_device(positions, shield, width, hardness, softness, coupling, pair_bits, right_side):
    nx, ny, nz, lanes = hardness.shape
    owned = nx * ny * nz
    ext = (nx + 2, ny + 2, nz + 2)
    tiles = ext[0] * ext[1] * ext[2]
    slots = owned * 27

    def kept(value):
        return pltpu.with_memory_space_constraint(value, pltpu.VMEM)

    def limits(size, **more):
        return pltpu.CompilerParams(vmem_limit_bytes=size, **more)

    param_ext, field_ext, field_own = pl.pallas_call(
        first_halo,
        out_shape=(
            pltpu.VMEM(ext + (8, lanes), F32),
            pltpu.VMEM(ext + (1, lanes), F32),
            pltpu.VMEM((nx, ny, nz, 4, lanes), F32),
        ),
        in_specs=[pl.BlockSpec(memory_space=pltpu.HBM)] * 4,
        out_specs=(VMEM_SPEC,) * 3,
        scratch_shapes=[
            pltpu.VMEM((nx, ny, nz, 8, lanes), F32),
            pltpu.VMEM((nx, ny, nz, 1, lanes), F32),
            pltpu.VMEM(positions.shape, F32),
            pltpu.VMEM(shield.shape, F32),
            pltpu.VMEM(width.shape, F32),
            pltpu.VMEM(right_side.shape, F32),
            pltpu.SemaphoreType.DMA((4,)),
            pltpu.SemaphoreType.DMA((2, 26)),
            pltpu.SemaphoreType.DMA((2, 26)),
        ],
        compiler_params=limits(4 << 20, collective_id=0, has_side_effects=True),
        name="first_halo",
    )(positions, shield, width, right_side)

    hard, soft, link = (a.reshape(owned // 8, 8, lanes) for a in (hardness, softness, coupling))
    own0 = field_own.reshape(owned, 4, lanes)
    vector = jax.ShapeDtypeStruct((owned, 4, lanes), F32)
    blank = pl.pallas_call(
        lambda ref: None,
        out_shape=pltpu.VMEM((slots, 2, lanes, lanes), BF),
        out_specs=VMEM_SPEC,
        compiler_params=limits(1 << 20),
        name="reserve",
    )()
    store, entries, count, diagonal, image0, own1 = pl.pallas_call(
        build,
        out_shape=(
            pltpu.VMEM((slots, 2, lanes, lanes), BF),
            jax.ShapeDtypeStruct((slots + 32,), jnp.int32),
            jax.ShapeDtypeStruct((1,), jnp.int32),
            jax.ShapeDtypeStruct((owned, 4, lanes), F32),
            jax.ShapeDtypeStruct((owned, 4, lanes), F32),
            jax.ShapeDtypeStruct((owned, 4, lanes), F32),
        ),
        in_specs=[SMEM_SPEC] + [VMEM_SPEC] * 7,
        input_output_aliases={7: 0},
        out_specs=(VMEM_SPEC, SMEM_SPEC, SMEM_SPEC, VMEM_SPEC, VMEM_SPEC, VMEM_SPEC),
        scratch_shapes=[
            pltpu.VMEM((tiles, lanes, lanes), BF),
            pltpu.VMEM((owned, 48, 2 * lanes), BF),
            pltpu.VMEM((tiles, 16, lanes), BF),
            pltpu.VMEM((owned + 1, 16, 2 * lanes), F32),
        ],
        compiler_params=limits(8 << 20),
        name="build",
    )(
        pair_bits,
        kept(param_ext.reshape(tiles, 8, lanes)),
        kept(field_ext.reshape(tiles, 1, lanes)),
        own0,
        hard,
        soft,
        link,
        kept(blank),
    )

    def halo(own, number):
        return pl.pallas_call(
            next_halo,
            out_shape=jax.ShapeDtypeStruct(ext + (4, lanes), F32),
            in_specs=[VMEM_SPEC],
            out_specs=VMEM_SPEC,
            scratch_shapes=[pltpu.SemaphoreType.DMA((1, 26)), pltpu.SemaphoreType.DMA((1, 26))],
            compiler_params=limits(2 << 20, collective_id=number, has_side_effects=True),
            name="halo",
        )(own.reshape(nx, ny, nz, 4, lanes))

    def operate(own, store, number):
        field = halo(own, number)
        return pl.pallas_call(
            again,
            out_shape=(
                jax.ShapeDtypeStruct((owned, 4, lanes), F32),
                jax.ShapeDtypeStruct((owned, 4, lanes), F32),
                pltpu.VMEM(store.shape, BF),
            ),
            in_specs=[VMEM_SPEC] * 4 + [SMEM_SPEC] * 2 + [VMEM_SPEC],
            out_specs=(VMEM_SPEC,) * 3,
            input_output_aliases={3: 2},
            scratch_shapes=[
                pltpu.VMEM((tiles, 16, lanes), BF),
                pltpu.VMEM((owned + 1, 8, 2 * lanes), F32),
            ],
            compiler_params=limits(4 << 20),
            name="apply",
        )(field.reshape(tiles, 4, lanes), own, link, kept(store), entries, count, diagonal)

    image1, own2, store = operate(own1, store, 1)
    image2, _, _ = operate(own2, store, 2)
    line = lax.axis_size("gx")
    plane = lax.axis_size("gy") * lax.axis_size("gz")
    shape = jax.ShapeDtypeStruct((4, owned // 8, 8, lanes), F32)
    answer, left = pl.pallas_call(
        combine,
        out_shape=(shape, shape),
        in_specs=[VMEM_SPEC] * 6,
        out_specs=(VMEM_SPEC, VMEM_SPEC),
        scratch_shapes=[
            pltpu.VMEM((2, 1, lanes), F32),
            pltpu.VMEM((plane, 1, lanes), F32),
            pltpu.VMEM((line, 1, lanes), F32),
            pltpu.SemaphoreType.DMA((2, plane - 1)),
            pltpu.SemaphoreType.DMA((2, plane - 1)),
        ],
        compiler_params=limits(4 << 20, collective_id=3, has_side_effects=True),
        name="combine",
    )(*(own0, own1, own2, image0, image1, image2))
    out = (4, nx, ny, nz, lanes)
    return answer.reshape(out), left.reshape(out)


def solution(mesh):
    tile = P("gx", "gy", "gz", None)
    field = P(None, "gx", "gy", "gz", None)
    return jax.shard_map(
        on_device,
        mesh=mesh,
        in_specs=(field, tile, tile, tile, tile, tile, P("gx", "gy", "gz"), field),
        out_specs=(field, field),
        check_vma=False,
    )
```

```python
import itertools

import jax
import jax.numpy as jnp
from jax import lax
from jax.experimental import pallas as pl
from jax.experimental.pallas import tpu as pltpu
from jax.sharding import PartitionSpec as P

MESH = pl.DeviceIdType.MESH
AXES = ("gx", "gy", "gz")
BF = jnp.bfloat16
F32 = jnp.float32
SHIFT = 4.0
LOG2E = 1.4426950408889634
COULOMB_GAIN = 250000.0
RESPONSE_SCALE = 0.003
GROUP = 32
WIDE = 32
DIRECTIONS = [d for d in itertools.product((-1, 0, 1), repeat=3) if d != (0, 0, 0)]
VMEM_SPEC = pl.BlockSpec(memory_space=pltpu.VMEM)
SMEM_SPEC = pl.BlockSpec(memory_space=pltpu.SMEM)


def own_range(step, size):
    return pl.ds(0, size) if step == 0 else pl.ds(size - 1 if step > 0 else 0, 1)


def ghost_range(step, size):
    return pl.ds(1, size) if step == 0 else pl.ds(0 if step > 0 else size + 1, 1)


def neighbour(direction):
    exists = None
    place = []
    for axis, step in zip(AXES, direction):
        at = lax.axis_index(axis) + step
        place.append(at)
        if step:
            inside = at >= 0 if step < 0 else at < lax.axis_size(axis)
            exists = inside if exists is None else exists & inside
    return tuple(place), exists


def greet():
    barrier = pltpu.get_barrier_semaphore()
    count = jnp.int32(0)
    for direction in DIRECTIONS:
        place, exists = neighbour(direction)

        @pl.when(exists)
        def _():
            pl.semaphore_signal(barrier, inc=1, device_id=place, device_id_type=MESH)

        count = count + exists.astype(jnp.int32)
    return barrier, count


def exchange(pairs, send_sem, recv_sem):
    def copies(index, direction, place):
        made = []
        for number, (own, ext) in enumerate(pairs):
            size = own.shape[:3]
            source = own.at[tuple(own_range(s, n) for s, n in zip(direction, size))]
            target = ext.at[tuple(ghost_range(s, n) for s, n in zip(direction, size))]
            made.append(
                pltpu.make_async_remote_copy(
                    source,
                    target,
                    send_sem.at[number, index],
                    recv_sem.at[number, index],
                    device_id=place,
                    device_id_type=MESH,
                )
            )
        return made

    for index, direction in enumerate(DIRECTIONS):
        place, exists = neighbour(direction)

        @pl.when(exists)
        def _():
            for copy in copies(index, direction, place):
                copy.start()

    for index, direction in enumerate(DIRECTIONS):
        place, exists = neighbour(direction)
        source, incoming = neighbour(tuple(-s for s in direction))

        @pl.when(incoming)
        def _():
            for copy in copies(index, direction, place):
                copy.wait_recv()

        @pl.when(exists)
        def _():
            for copy in copies(index, direction, place):
                copy.wait_send()


def first_halo(pos_in, shield_in, width_in, rhs_in, param_ext, field_ext, *scratch):
    param_own, last_own, pos, shield, width, rhs, load_sem, send_sem, recv_sem = scratch
    loads = [
        pltpu.make_async_copy(source, target, load_sem.at[index])
        for index, (source, target) in enumerate(
            ((pos_in, pos), (shield_in, shield), (width_in, width), (rhs_in, rhs))
        )
    ]
    for load in loads:
        load.start()
    param_ext[...] = jnp.zeros_like(param_ext)
    field_ext[...] = jnp.zeros_like(field_ext)
    barrier, count = greet()
    for load in loads:
        load.wait()
    nx, ny, nz = param_own.shape[:3]
    for x in range(nx):
        for y in range(ny):
            columns = [pos[0, x, y], pos[1, x, y], pos[2, x, y], shield[x, y], width[x, y]]
            columns = columns + [rhs[f, x, y] for f in range(4)]
            for z in range(nz):
                for f in range(9):
                    row = columns[f][z : z + 1]
                    if f < 8:
                        param_own[x, y, z, f : f + 1, :] = row
                        param_ext[x + 1, y + 1, z + 1, f : f + 1, :] = row
                    else:
                        last_own[x, y, z] = row
                        field_ext[x + 1, y + 1, z + 1] = row
    pl.semaphore_wait(barrier, count)
    exchange(((param_own, param_ext), (last_own, field_ext)), send_sem, recv_sem)


def next_halo(own, ext, send_sem, recv_sem):
    ext[...] = jnp.zeros_like(ext)
    barrier, count = greet()
    ext[1:-1, 1:-1, 1:-1] = own[...]
    pl.semaphore_wait(barrier, count)
    exchange(((own, ext),), send_sem, recv_sem)


def split3(value):
    first = value.astype(BF)
    rest = value - first.astype(F32)
    second = rest.astype(BF)
    third = (rest - second.astype(F32)).astype(BF)
    return first.astype(F32), second.astype(F32), third.astype(F32)


def rows_of(pieces):
    row = lax.broadcasted_iota(jnp.int32, (8, 128), 0)
    value = jnp.zeros((8, 128), F32)
    for index, piece in pieces:
        value = jnp.where(row == index, piece, value)
    return value


def centred(param, ex, ey, ez, half):
    row = lax.broadcasted_iota(jnp.int32, (8, 128), 0)
    offset = jnp.where(row == 0, ex, jnp.where(row == 1, ey, ez)).astype(F32) - jnp.where(
        row == 0, half[0], jnp.where(row == 1, half[1], half[2])
    )
    place = param + offset
    square = jnp.sum(jnp.where(row < 3, place * place, 0.0), axis=0, keepdims=True)
    return row, place, jnp.broadcast_to(square, (8, 128))


def partner_features(param, ex, ey, ez, half):
    row, place, square = centred(param, ex, ey, ez, half)
    value = jnp.where(row < 3, place, jnp.where(row == 3, param, 0.0))
    value = jnp.where(row == 4, square, jnp.where(row == 5, 1.0, value))
    one, two, three = split3(value)
    return jnp.concatenate([one, two, one, two, three, one], axis=0)


def own_features(param, ex, ey, ez, half):
    row, place, square = centred(param, ex, ey, ez, half)
    sides = []
    for gain, shielded in ((-LOG2E, 0.0), (COULOMB_GAIN, COULOMB_GAIN)):
        value = jnp.where(row < 3, (-2.0 * gain) * place, jnp.where(row == 3, shielded * param, 0.0))
        value = jnp.where(row == 4, gain, jnp.where(row == 5, gain * square, value))
        one, two, three = split3(value)
        sides.append(jnp.concatenate([one, one, two, two, one, three], axis=0))
    return jnp.concatenate(sides, axis=1)


def split_fields(load, halves, tiles):
    ones = jnp.ones((8, 128), F32)

    def step(index, carry):
        values = [load(index * 16 + sub) for sub in range(16)]
        parts = []
        for value in values:
            high = value.astype(BF).astype(F32)
            parts.append(jnp.concatenate([high, value - high, ones], axis=0).astype(BF))
        for sub in range(16):
            halves[index * 16 + sub] = parts[sub]
        return carry

    lax.fori_loop(0, tiles // 16, step, 0)


def apply_group(base, size, entries, halves, window, acc):
    rows = acc.shape[1]
    for sub in range(size):
        code = entries[base + sub]
        e = code & 255
        t = lax.shift_right_logical(code, 16)
        both = jnp.concatenate([window[sub, 0], window[sub, 1]], axis=1)
        out = jnp.dot(halves[e], both, preferred_element_type=F32)
        acc[t] = acc[t] + out[:rows]


def image_rows(out, diagonal, link, value):
    row = lax.broadcasted_iota(jnp.int32, (4, 128), 0)
    summed = out[0:4] + out[4:8]
    pair = jnp.where(row < 2, summed[:, :128], -summed[:, 128:])
    swapped = jnp.concatenate([value[2:4], value[0:2]], axis=0)
    return diagonal * value + pair + link * swapped


def finish_all(owned, make):
    def step(index, carry):
        results = [make(index, sub) for sub in range(8)]
        for sub, (targets, values) in enumerate(results):
            for target, value in zip(targets, values):
                target[index * 8 + sub] = value
        return carry

    lax.fori_loop(0, owned // 8, step, 0)


def build(
    bits, param, field, hardness, softness, coupling, blank, store, entries, count, diagonal, image, own, send,
    features, mine, halves, acc
):
    ey_size, ez_size = 4, 10
    half = (2.0, 2.0, 5.0)
    tiles = 160
    owned = 32

    def place_of(t):
        return ((t // 16 + 1) * ey_size + t // 8 % 2 + 1) * ez_size + t % 8 + 1

    def features_step(index, at):
        ex = lax.shift_right_logical(index, 2)
        ey = index & 3
        loaded = [param[index * ez_size + ez] for ez in range(ez_size)]
        made = [partner_features(loaded[ez], ex, ey, ez, half).T.astype(BF) for ez in range(ez_size)]
        for ez in range(ez_size):
            features[index * ez_size + ez, :, 0:48] = made[ez]
        for sub in range(2):
            t = index * 2 + sub
            x = lax.shift_right_logical(t, 4)
            y = lax.shift_right_logical(t, 3) & 1
            z = t & 7
            word = bits[x, y, z]
            own_code = ((x + 1) * ey_size + y + 1) * ez_size + z + 1 + 65792 * t
            entries[t] = own_code
            for code in range(27):
                if code == 13:
                    continue
                shift = ((code // 9 - 1) * ey_size + (code // 3 % 3 - 1)) * ez_size + code % 3 - 1
                entries[at] = own_code + shift
                at = at + (lax.shift_right_logical(word, code) & 1)
        return at

    total = lax.fori_loop(0, 16, features_step, jnp.int32(owned))
    middle = (ey_size + 1) * ez_size + 1
    for sub in range(WIDE):
        entries[total + sub] = middle + 65536 * owned
    count[0] = total

    def own_step(index, carry):
        ex = lax.shift_right_logical(index, 1) + 1
        ey = (index & 1) + 1
        first = (ex * ey_size + ey) * ez_size + 1
        made = [own_features(param[first + z], ex, ey, z + 1, half).astype(BF) for z in range(8)]
        for z in range(8):
            mine[index * 8 + z] = made[z]
        return carry

    lax.fori_loop(0, owned // 8, own_step, 0)
    split_fields(lambda e: jnp.concatenate([param[e, 5:8, :], field[e]], axis=0), halves, tiles)
    acc[...] = jnp.zeros_like(acc)

    def pair(slot, window, sub, masked):
        code = entries[slot]
        e = code & 255
        t = lax.shift_right_logical(code, 8) & 255
        both = jnp.dot(features[e, :, 0:48], mine[t], preferred_element_type=F32)
        partner_width = jnp.broadcast_to(param[e, 4:5, :], (128, 128)).T
        widths = partner_width + param[place_of(t), 4:5, :]
        coulomb = lax.rsqrt(both[:, 128:])
        response = RESPONSE_SCALE * jnp.exp2(both[:, :128] / widths)
        if masked:
            same = lax.broadcasted_iota(jnp.int32, (128, 128), 0) == lax.broadcasted_iota(
                jnp.int32, (128, 128), 1
            )
            coulomb = jnp.where(same, 0.0, coulomb)
            response = jnp.where(same, 0.0, response)
        window[sub, 0] = coulomb.astype(BF)
        window[sub, 1] = response.astype(BF)

    def self_step(index, carry):
        window = store.at[pl.ds(index * 8, 8)]
        for sub in range(8):
            pair(index * 8 + sub, window, sub, True)
        return carry

    lax.fori_loop(0, owned // 8, self_step, 0)
    apply_group(0, owned - GROUP, entries, halves, store, acc)

    def pair_step(index, carry):
        base = owned + index * GROUP
        window = store.at[pl.ds(base - GROUP, 2 * GROUP)]
        apply_group(base - GROUP, GROUP, entries, halves, window, acc)
        for sub in range(GROUP):
            pair(base + sub, window, GROUP + sub, False)
        return carry

    groups = (total - owned + GROUP - 1) // GROUP
    lax.fori_loop(0, groups, pair_step, 0)
    last = owned + (groups - 1) * GROUP
    apply_group(last, GROUP, entries, halves, store.at[pl.ds(last, GROUP)], acc)
    row = lax.broadcasted_iota(jnp.int32, (4, 128), 0)

    def make(index, sub):
        out = acc[index * 8 + sub]
        e = place_of(index * 8) + sub
        value = jnp.concatenate([param[e, 5:8, :], field[e]], axis=0)
        top = hardness[index, sub : sub + 1, :] + out[8:9, :128]
        low = softness[index, sub : sub + 1, :] + out[8:9, 128:]
        diag = jnp.where(row < 2, top, low)
        made = image_rows(out, diag, coupling[index, sub : sub + 1, :], value)
        return (diagonal, image, own, send), (diag, made, value, made - SHIFT * value)

    finish_all(owned, make)


def again(field, own, coupling, store, entries, count, diagonal, unused, idle, image, send, passed, halves, acc):
    owned = 32
    split_fields(lambda e: field[e], halves, field.shape[0])
    acc[...] = jnp.zeros_like(acc)

    def step(index, carry):
        apply_group(index * WIDE, WIDE, entries, halves, store.at[pl.ds(index * WIDE, WIDE)], acc)
        return carry

    lax.fori_loop(0, (count[0] + WIDE - 1) // WIDE, step, 0)

    def make(index, sub):
        value = own[index * 8 + sub]
        diag = diagonal[index * 8 + sub]
        made = image_rows(acc[index * 8 + sub], diag, coupling[index, sub : sub + 1, :], value)
        return (image, send), (made, made - SHIFT * value)

    finish_all(owned, make)


def combine(u0, u1, u2, w0, w1, w2, solution, residual, part, plane, line, send_sem, recv_sem):
    sizes = [lax.axis_size(axis) for axis in AXES]
    gx, gy, gz = (lax.axis_index(axis) for axis in AXES)
    across = []
    for a in range(sizes[1]):
        for b in range(sizes[2]):
            if a or b:
                across.append((gx, lax.rem(gy + a, sizes[1]), lax.rem(gz + b, sizes[2])))
    along = [(lax.rem(gx + a, sizes[0]), gy, gz) for a in range(1, sizes[0])]
    barrier = pltpu.get_barrier_semaphore()
    for peer in across + along:
        pl.semaphore_signal(barrier, inc=1, device_id=peer, device_id_type=MESH)

    wanted = [(u0, u0), (u0, u1), (u0, u2), (u0, w0), (u0, w1), (u0, w2), (u1, w1), (u1, w2), (u2, w2)]
    sums = []
    for left, right in wanted:
        both = jnp.sum(left[...] * right[...], axis=0)
        sums.append(both[0:2] + both[2:4])
    stacked = jnp.concatenate(sums + [jnp.zeros((128 - 18, 128), F32)], axis=0)
    part[0] = jnp.sum(stacked.T, axis=0, keepdims=True)
    pl.semaphore_wait(barrier, len(across) + len(along))

    def gather(turn, peers, here, stage, width):
        made = []
        for index, peer in enumerate(peers):
            copy = pltpu.make_async_remote_copy(
                part.at[turn],
                stage.at[here],
                send_sem.at[turn, index],
                recv_sem.at[turn, index],
                device_id=peer,
                device_id_type=MESH,
            )
            copy.start()
            made.append(copy)
        stage[here] = part[turn]
        for copy in made:
            copy.wait_recv()
        total = jnp.sum(stage[...], axis=0)
        for copy in made:
            copy.wait_send()
        return total

    part[1] = gather(0, across, gy * sizes[2] + gz, plane, len(across) + 1)
    total = gather(1, along, gx, line, len(along) + 1)
    m0, m1, m2, g00, g01, g02, g11, g12, g22 = (total[:, 2 * k : 2 * k + 2] for k in range(9))
    f1 = g01 / g00
    f2 = g02 / g00
    h11 = g11 - f1 * g01
    h12 = g12 - f1 * g02
    h22 = g22 - f2 * g02
    n1 = m1 - f1 * m0
    n2 = m2 - f2 * m0
    f3 = h12 / h11
    k22 = h22 - f3 * h12
    k2 = n2 - f3 * n1
    c2 = k2 / k22
    c1 = (n1 - h12 * c2) / h11
    c0 = (m0 - g01 * c1 - g02 * c2) / g00

    def spread(c):
        pair = [jnp.broadcast_to(c[:, r : r + 1], (1, 128)) for r in range(2)]
        return jnp.concatenate(pair + pair, axis=0)[None]

    c0, c1, c2 = (spread(c) for c in (c0, c1, c2))
    answer = c0 * u0[...] + c1 * u1[...] + c2 * u2[...]
    left = u0[...] - (c0 * w0[...] + c1 * w1[...] + c2 * w2[...])
    for t in range(32):
        for f in range(4):
            solution[f, t // 8, t % 8 : t % 8 + 1, :] = answer[t, f : f + 1]
            residual[f, t // 8, t % 8 : t % 8 + 1, :] = left[t, f : f + 1]


def on_device(positions, shield, width, hardness, softness, coupling, pair_bits, right_side):
    nx, ny, nz, lanes = hardness.shape
    owned = nx * ny * nz
    ext = (nx + 2, ny + 2, nz + 2)
    tiles = ext[0] * ext[1] * ext[2]
    slots = owned * 27

    def kept(value):
        return pltpu.with_memory_space_constraint(value, pltpu.VMEM)

    def far(value):
        return pltpu.with_memory_space_constraint(value, pltpu.HBM)

    def limits(size, **more):
        return pltpu.CompilerParams(vmem_limit_bytes=size, **more)

    param_ext, field_ext = pl.pallas_call(
        first_halo,
        out_shape=(
            pltpu.VMEM(ext + (8, lanes), F32),
            pltpu.VMEM(ext + (1, lanes), F32),
        ),
        in_specs=[pl.BlockSpec(memory_space=pltpu.HBM)] * 4,
        out_specs=(VMEM_SPEC,) * 2,
        scratch_shapes=[
            pltpu.VMEM((nx, ny, nz, 8, lanes), F32),
            pltpu.VMEM((nx, ny, nz, 1, lanes), F32),
            pltpu.VMEM(positions.shape, F32),
            pltpu.VMEM(shield.shape, F32),
            pltpu.VMEM(width.shape, F32),
            pltpu.VMEM(right_side.shape, F32),
            pltpu.SemaphoreType.DMA((4,)),
            pltpu.SemaphoreType.DMA((2, 26)),
            pltpu.SemaphoreType.DMA((2, 26)),
        ],
        compiler_params=limits(4 << 20, collective_id=0, has_side_effects=True),
        name="first_halo",
    )(*(far(a) for a in (positions, shield, width, right_side)))

    hard, soft, link = (a.reshape(owned // 8, 8, lanes) for a in (hardness, softness, coupling))
    vector = jax.ShapeDtypeStruct((owned, 4, lanes), F32)
    blank = pl.pallas_call(
        lambda ref: None,
        out_shape=pltpu.VMEM((slots, 2, lanes, lanes), BF),
        out_specs=VMEM_SPEC,
        compiler_params=limits(8 << 20),
        name="reserve",
    )()
    store, entries, count, diagonal, image0, own0, own1 = pl.pallas_call(
        build,
        out_shape=(
            pltpu.VMEM((slots, 2, lanes, lanes), BF),
            jax.ShapeDtypeStruct((slots + 32,), jnp.int32),
            jax.ShapeDtypeStruct((1,), jnp.int32),
            pltpu.VMEM((owned, 4, lanes), F32),
            pltpu.VMEM((owned, 4, lanes), F32),
            pltpu.VMEM((owned, 4, lanes), F32),
            pltpu.VMEM((owned, 4, lanes), F32),
        ),
        in_specs=[SMEM_SPEC] + [VMEM_SPEC] * 6,
        input_output_aliases={6: 0},
        out_specs=(VMEM_SPEC, SMEM_SPEC, SMEM_SPEC) + (VMEM_SPEC,) * 4,
        scratch_shapes=[
            pltpu.VMEM((tiles, lanes, lanes), BF),
            pltpu.VMEM((owned, 48, 2 * lanes), BF),
            pltpu.VMEM((tiles, 16, lanes), BF),
            pltpu.VMEM((owned + 1, 16, 2 * lanes), F32),
        ],
        compiler_params=limits(8 << 20),
        name="build",
    )(
        pair_bits,
        kept(param_ext.reshape(tiles, 8, lanes)),
        kept(field_ext.reshape(tiles, 1, lanes)),
        hard,
        soft,
        link,
        kept(blank),
    )

    def halo(own, number):
        return pl.pallas_call(
            next_halo,
            out_shape=pltpu.VMEM(ext + (4, lanes), F32),
            in_specs=[VMEM_SPEC],
            out_specs=VMEM_SPEC,
            scratch_shapes=[pltpu.SemaphoreType.DMA((1, 26)), pltpu.SemaphoreType.DMA((1, 26))],
            compiler_params=limits(2 << 20, collective_id=number, has_side_effects=True),
            name="halo",
        )(kept(own.reshape(nx, ny, nz, 4, lanes)))

    def operate(own, store, number):
        field = halo(own, number)
        return pl.pallas_call(
            again,
            out_shape=(
                pltpu.VMEM((owned, 4, lanes), F32),
                pltpu.VMEM((owned, 4, lanes), F32),
                pltpu.VMEM(store.shape, BF),
            ),
            in_specs=[VMEM_SPEC] * 4 + [SMEM_SPEC] * 2 + [VMEM_SPEC] * 3,
            out_specs=(VMEM_SPEC,) * 3,
            input_output_aliases={3: 2},
            scratch_shapes=[
                pltpu.VMEM((tiles, 16, lanes), BF),
                pltpu.VMEM((owned + 1, 8, 2 * lanes), F32),
            ],
            compiler_params=limits(8 << 20),
            name="apply",
        )(kept(field.reshape(tiles, 4, lanes)), kept(own), link, kept(store), entries, count, kept(diagonal), kept(param_ext), kept(field_ext))

    image1, own2, store = operate(own1, store, 1)
    image2, _, _ = operate(own2, store, 2)
    line = lax.axis_size("gx")
    plane = lax.axis_size("gy") * lax.axis_size("gz")
    shape = jax.ShapeDtypeStruct((4, owned // 8, 8, lanes), F32)
    answer, left = pl.pallas_call(
        combine,
        out_shape=(shape, shape),
        in_specs=[VMEM_SPEC] * 6,
        out_specs=(VMEM_SPEC, VMEM_SPEC),
        scratch_shapes=[
            pltpu.VMEM((2, 1, lanes), F32),
            pltpu.VMEM((plane, 1, lanes), F32),
            pltpu.VMEM((line, 1, lanes), F32),
            pltpu.SemaphoreType.DMA((2, plane - 1)),
            pltpu.SemaphoreType.DMA((2, plane - 1)),
        ],
        compiler_params=limits(4 << 20, collective_id=3, has_side_effects=True),
        name="combine",
    )(*(kept(a) for a in (own0, own1, own2, image0, image1, image2)))
    out = (4, nx, ny, nz, lanes)
    return answer.reshape(out), left.reshape(out)


def solution(mesh):
    tile = P("gx", "gy", "gz", None)
    field = P(None, "gx", "gy", "gz", None)
    return jax.shard_map(
        on_device,
        mesh=mesh,
        in_specs=(field, tile, tile, tile, tile, tile, P("gx", "gy", "gz"), field),
        out_specs=(field, field),
        check_vma=False,
    )
```

```python
import itertools

import jax
import jax.numpy as jnp
from jax import lax
from jax.experimental import pallas as pl
from jax.experimental.pallas import tpu as pltpu
from jax.sharding import PartitionSpec as P

MESH = pl.DeviceIdType.MESH
AXES = ("gx", "gy", "gz")
BF = jnp.bfloat16
F32 = jnp.float32
SHIFT = 4.0
LOG2E = 1.4426950408889634
COULOMB_GAIN = 250000.0
RESPONSE_SCALE = 0.003
GROUP = 32
LIMIT = 8 << 20
DIRECTIONS = [d for d in itertools.product((-1, 0, 1), repeat=3) if d != (0, 0, 0)]
VMEM_SPEC = pl.BlockSpec(memory_space=pltpu.VMEM)
SMEM_SPEC = pl.BlockSpec(memory_space=pltpu.SMEM)


def own_range(step, size):
    return pl.ds(0, size) if step == 0 else pl.ds(size - 1 if step > 0 else 0, 1)


def ghost_range(step, size):
    return pl.ds(1, size) if step == 0 else pl.ds(0 if step > 0 else size + 1, 1)


def neighbour(direction):
    exists = None
    place = []
    for axis, step in zip(AXES, direction):
        at = lax.axis_index(axis) + step
        place.append(at)
        if step:
            inside = at >= 0 if step < 0 else at < lax.axis_size(axis)
            exists = inside if exists is None else exists & inside
    return tuple(place), exists


def greet():
    barrier = pltpu.get_barrier_semaphore()
    count = jnp.int32(0)
    for direction in DIRECTIONS:
        place, exists = neighbour(direction)

        @pl.when(exists)
        def _():
            pl.semaphore_signal(barrier, inc=1, device_id=place, device_id_type=MESH)

        count = count + exists.astype(jnp.int32)
    return barrier, count


def rim_copies(pairs, index, direction, place, send_sem, recv_sem):
    made = []
    for number, (own, ext) in enumerate(pairs):
        size = own.shape[:3]
        made.append(
            pltpu.make_async_remote_copy(
                own.at[tuple(own_range(s, n) for s, n in zip(direction, size))],
                ext.at[tuple(ghost_range(s, n) for s, n in zip(direction, size))],
                send_sem.at[number, index],
                recv_sem.at[number, index],
                device_id=place,
                device_id_type=MESH,
            )
        )
    return made


def send_rims(pairs, send_sem, recv_sem):
    for index, direction in enumerate(DIRECTIONS):
        place, exists = neighbour(direction)

        @pl.when(exists)
        def _():
            for copy in rim_copies(pairs, index, direction, place, send_sem, recv_sem):
                copy.start()


def await_rims(pairs, send_sem, recv_sem):
    for index, direction in enumerate(DIRECTIONS):
        place, exists = neighbour(direction)
        source, incoming = neighbour(tuple(-s for s in direction))

        @pl.when(incoming)
        def _():
            for copy in rim_copies(pairs, index, direction, place, send_sem, recv_sem):
                copy.wait_recv()

        @pl.when(exists)
        def _():
            for copy in rim_copies(pairs, index, direction, place, send_sem, recv_sem):
                copy.wait_send()


def first_halo(pos_in, shield_in, width_in, rhs_in, param_ext, field_ext, store, *scratch):
    param_own, last_own, pos, shield, width, rhs, load_sem, send_sem, recv_sem = scratch
    loads = [
        pltpu.make_async_copy(source, target, load_sem.at[index])
        for index, (source, target) in enumerate(
            ((pos_in, pos), (shield_in, shield), (width_in, width), (rhs_in, rhs))
        )
    ]
    for load in loads:
        load.start()
    param_ext[...] = jnp.zeros_like(param_ext)
    field_ext[...] = jnp.zeros_like(field_ext)
    barrier, count = greet()
    for load in loads:
        load.wait()
    nx, ny, nz = param_own.shape[:3]
    for x in range(nx):
        for y in range(ny):
            columns = [pos[0, x, y], pos[1, x, y], pos[2, x, y], shield[x, y], width[x, y]]
            columns = columns + [rhs[f, x, y] for f in range(4)]
            for z in range(nz):
                for f in range(9):
                    row = columns[f][z : z + 1]
                    if f < 8:
                        param_own[x, y, z, f : f + 1, :] = row
                        param_ext[x + 1, y + 1, z + 1, f : f + 1, :] = row
                    else:
                        last_own[x, y, z] = row
                        field_ext[x + 1, y + 1, z + 1] = row
    pl.semaphore_wait(barrier, count)
    pairs = ((param_own, param_ext), (last_own, field_ext))
    send_rims(pairs, send_sem, recv_sem)
    slots = store.shape[0]

    def clear(index, carry):
        store[pl.ds(index * 5, 5)] = jnp.zeros((5,) + store.shape[1:], BF)
        return carry

    lax.fori_loop(0, slots // 5, clear, 0)
    await_rims(pairs, send_sem, recv_sem)


def split3(value):
    first = value.astype(BF)
    rest = value - first.astype(F32)
    second = rest.astype(BF)
    third = (rest - second.astype(F32)).astype(BF)
    return first.astype(F32), second.astype(F32), third.astype(F32)


def rows_of(pieces):
    row = lax.broadcasted_iota(jnp.int32, (8, 128), 0)
    value = jnp.zeros((8, 128), F32)
    for index, piece in pieces:
        value = jnp.where(row == index, piece, value)
    return value


def centred(param, ex, ey, ez, half):
    row = lax.broadcasted_iota(jnp.int32, (8, 128), 0)
    offset = jnp.where(row == 0, ex, jnp.where(row == 1, ey, ez)).astype(F32) - jnp.where(
        row == 0, half[0], jnp.where(row == 1, half[1], half[2])
    )
    place = param + offset
    square = jnp.sum(jnp.where(row < 3, place * place, 0.0), axis=0, keepdims=True)
    return row, place, jnp.broadcast_to(square, (8, 128))


def partner_features(param, ex, ey, ez, half):
    row, place, square = centred(param, ex, ey, ez, half)
    value = jnp.where(row < 3, place, jnp.where(row == 3, param, 0.0))
    value = jnp.where(row == 4, square, jnp.where(row == 5, 1.0, value))
    one, two, three = split3(value)
    return jnp.concatenate([one, two, one, two, three, one], axis=0)


def own_features(param, ex, ey, ez, half):
    row, place, square = centred(param, ex, ey, ez, half)
    sides = []
    for gain, shielded in ((-LOG2E, 0.0), (COULOMB_GAIN, COULOMB_GAIN)):
        value = jnp.where(row < 3, (-2.0 * gain) * place, jnp.where(row == 3, shielded * param, 0.0))
        value = jnp.where(row == 4, gain, jnp.where(row == 5, gain * square, value))
        one, two, three = split3(value)
        sides.append(jnp.concatenate([one, one, two, two, one, three], axis=0))
    return jnp.concatenate(sides, axis=1)


def split_fields(load, halves, tiles):
    ones = jnp.ones((8, 128), F32)

    def step(index, carry):
        values = [load(index * 16 + sub) for sub in range(16)]
        parts = []
        for value in values:
            high = value.astype(BF).astype(F32)
            parts.append(jnp.concatenate([high, value - high, ones], axis=0).astype(BF))
        for sub in range(16):
            halves[index * 16 + sub] = parts[sub]
        return carry

    lax.fori_loop(0, tiles // 16, step, 0)


def apply_group(base, size, entries, halves, store, acc):
    for sub in range(size):
        code = entries[base + sub]
        e = code & 255
        t = lax.shift_right_logical(code, 14) & 63
        slot = lax.shift_right_logical(code, 20)
        both = jnp.concatenate([store[slot, 0], store[slot, 1]], axis=1)
        acc[t] = acc[t] + jnp.dot(halves[e], both, preferred_element_type=F32)


def image_rows(out, diagonal, link, value):
    row = lax.broadcasted_iota(jnp.int32, (4, 128), 0)
    summed = out[0:4] + out[4:8]
    pair = jnp.where(row < 2, summed[:, :128], -summed[:, 128:])
    swapped = jnp.concatenate([value[2:4], value[0:2]], axis=0)
    return diagonal * value + pair + link * swapped


def finish_all(owned, make):
    def step(index, carry):
        results = [make(index, sub) for sub in range(8)]
        for sub, (targets, values) in enumerate(results):
            for target, value in zip(targets, values):
                target[index * 8 + sub] = value
        return carry

    lax.fori_loop(0, owned // 8, step, 0)


def build(
    bits, param, field, hardness, softness, coupling, blank, store, diagonal, image, own, send,
    features, mine, halves, acc, entries
):
    ey_size, ez_size = 4, 10
    half = (2.0, 2.0, 5.0)
    tiles = 160
    owned = 32

    def place_of(t):
        return ((t // 16 + 1) * ey_size + t // 8 % 2 + 1) * ez_size + t % 8 + 1

    def features_step(index, at):
        ex = lax.shift_right_logical(index, 2)
        ey = index & 3
        loaded = [param[index * ez_size + ez] for ez in range(ez_size)]
        made = [partner_features(loaded[ez], ex, ey, ez, half).T.astype(BF) for ez in range(ez_size)]
        for ez in range(ez_size):
            features[index * ez_size + ez, :, 0:48] = made[ez]
        for sub in range(2):
            t = index * 2 + sub
            x = lax.shift_right_logical(t, 4)
            y = lax.shift_right_logical(t, 3) & 1
            z = t & 7
            word = bits[x, y, z]
            own_code = ((x + 1) * ey_size + y + 1) * ez_size + z + 1 + 256 * t + 16384 * t + (27 << 20) * t
            entries[t] = own_code + (13 << 20)
            for code in range(27):
                if code == 13:
                    continue
                shift = ((code // 9 - 1) * ey_size + (code // 3 % 3 - 1)) * ez_size + code % 3 - 1
                entries[at] = own_code + shift + (code << 20)
                at = at + (lax.shift_right_logical(word, code) & 1)
        return at

    total = lax.fori_loop(0, 16, features_step, jnp.int32(owned))
    middle = (ey_size + 1) * ez_size + 1
    for sub in range(GROUP):
        entries[total + sub] = middle + 16384 * owned + ((27 * owned) << 20)

    def own_step(index, carry):
        ex = lax.shift_right_logical(index, 1) + 1
        ey = (index & 1) + 1
        first = (ex * ey_size + ey) * ez_size + 1
        made = [own_features(param[first + z], ex, ey, z + 1, half).astype(BF) for z in range(8)]
        for z in range(8):
            mine[index * 8 + z] = made[z]
        return carry

    lax.fori_loop(0, owned // 8, own_step, 0)
    split_fields(lambda e: jnp.concatenate([param[e, 5:8, :], field[e]], axis=0), halves, tiles)
    acc[...] = jnp.zeros_like(acc)

    def pair(position, masked):
        code = entries[position]
        e = code & 255
        t = lax.shift_right_logical(code, 8) & 63
        slot = lax.shift_right_logical(code, 20)
        both = jnp.dot(features[e, :, 0:48], mine[t], preferred_element_type=F32)
        partner_width = jnp.broadcast_to(param[e, 4:5, :], (128, 128)).T
        widths = partner_width + param[place_of(t), 4:5, :]
        coulomb = lax.rsqrt(both[:, 128:])
        response = RESPONSE_SCALE * jnp.exp2(both[:, :128] / widths)
        if masked:
            same = lax.broadcasted_iota(jnp.int32, (128, 128), 0) == lax.broadcasted_iota(
                jnp.int32, (128, 128), 1
            )
            coulomb = jnp.where(same, 0.0, coulomb)
            response = jnp.where(same, 0.0, response)
        store[slot, 0] = coulomb.astype(BF)
        store[slot, 1] = response.astype(BF)

    def self_step(index, carry):
        for sub in range(8):
            pair(index * 8 + sub, True)
        return carry

    lax.fori_loop(0, owned // 8, self_step, 0)
    apply_group(0, owned - GROUP, entries, halves, store, acc)

    def pair_step(index, carry):
        base = owned + index * GROUP
        apply_group(base - GROUP, GROUP, entries, halves, store, acc)
        for sub in range(GROUP):
            pair(base + sub, False)
        return carry

    groups = (total - owned + GROUP - 1) // GROUP
    lax.fori_loop(0, groups, pair_step, 0)
    last = owned + (groups - 1) * GROUP
    apply_group(last, GROUP, entries, halves, store, acc)
    row = lax.broadcasted_iota(jnp.int32, (4, 128), 0)

    def make(index, sub):
        out = acc[index * 8 + sub]
        e = place_of(index * 8) + sub
        value = jnp.concatenate([param[e, 5:8, :], field[e]], axis=0)
        top = hardness[index, sub : sub + 1, :] + out[8:9, :128]
        low = softness[index, sub : sub + 1, :] + out[8:9, 128:]
        diag = jnp.where(row < 2, top, low)
        made = image_rows(out, diag, coupling[index, sub : sub + 1, :], value)
        return (diagonal, image, own, send), (diag, made, value, made - SHIFT * value)

    finish_all(owned, make)


INSIDE = {0: (0, 1), 1: (-1, 0)}
FLAT = list(itertools.product((-1, 0, 1), repeat=2))


def solve(u0, u1, w0, diagonal, coupling, store, unused, idle, solution, residual, *scratch):
    ext1, ext2, u2, w1, w2, halves, acc, part, plane, line, rim_send, rim_recv, send_sem, recv_sem = scratch
    nx, ny, nz = u1.shape[:3]
    ey_size, ez_size = ny + 2, nz + 2
    sizes = [lax.axis_size(axis) for axis in AXES]
    gx, gy, gz = (lax.axis_index(axis) for axis in AXES)
    across = []
    for a in range(sizes[1]):
        for b in range(sizes[2]):
            if a or b:
                across.append((gx, lax.rem(gy + a, sizes[1]), lax.rem(gz + b, sizes[2])))
    along = [(lax.rem(gx + a, sizes[0]), gy, gz) for a in range(1, sizes[0])]
    ext1[...] = jnp.zeros_like(ext1)
    ext2[...] = jnp.zeros_like(ext2)
    barrier, count = greet()
    for peer in across + along:
        pl.semaphore_signal(barrier, inc=1, device_id=peer, device_id_type=MESH)

    def split_columns(ext, lowest, columns, rows, depth):
        def step(index, carry):
            x = index // columns + lowest
            y = index % columns + lowest
            values = [ext[x, y, z] for z in depth]
            parts = []
            for value in values:
                high = value.astype(BF).astype(F32)
                parts.append(jnp.concatenate([high, value - high, jnp.zeros((8, 128), F32)], axis=0).astype(BF))
            for z, made in zip(depth, parts):
                halves[(x * ey_size + y) * ez_size + z] = made
            return carry

        lax.fori_loop(0, columns * rows, step, 0)

    def tile_sum(x, y, z, offsets):
        total = None
        for dx, dy, dz in offsets:
            slot = ((x * ny + y) * nz + z) * 27 + (dx + 1) * 9 + (dy + 1) * 3 + dz + 1
            e = ((x + 1 + dx) * ey_size + y + 1 + dy) * ez_size + z + 1 + dz
            both = jnp.concatenate([store[slot, 0], store[slot, 1]], axis=1)
            out = jnp.dot(halves[e], both, preferred_element_type=F32)
            total = out if total is None else total + out
        return total[:8]

    columns = [(x, y) for x in range(nx) for y in range(ny)]

    def inside(x, y):
        return [(dx, dy) for dx in INSIDE[x] for dy in INSIDE[y]]

    def outside(x, y):
        return [d for d in FLAT if d not in inside(x, y)]

    def level_pass():
        def step(index, carry):
            for sub in range(2):
                z = index * 2 + sub
                for x, y in columns:
                    acc[(x * ny + y) * nz + z] = tile_sum(x, y, z, [d + (0,) for d in inside(x, y)])
            return carry

        lax.fori_loop(0, nz // 2, step, 0)

    def between_pass():
        def step(z, carry):
            for x, y in columns:
                t = (x * ny + y) * nz + z
                acc[t] = acc[t] + tile_sum(x, y, z, [d + (1,) for d in inside(x, y)])
                acc[t + 1] = acc[t + 1] + tile_sum(x, y, z + 1, [d + (-1,) for d in inside(x, y)])
            return carry

        lax.fori_loop(0, nz - 1, step, 0)

    def rim_pass():
        for x, y in columns:
            for z, dz in ((0, -1), (nz - 1, 1)):
                t = (x * ny + y) * nz + z
                acc[t] = acc[t] + tile_sum(x, y, z, [d + (dz,) for d in inside(x, y)])

        def step(index, carry):
            for sub in range(2):
                z = index * 2 + sub
                for x, y in columns:
                    t = (x * ny + y) * nz + z
                    around = [d + (dz,) for d in outside(x, y) for dz in (-1, 0, 1)]
                    acc[t] = acc[t] + tile_sum(x, y, z, around)
            return carry

        lax.fori_loop(0, nz // 2, step, 0)

    def finish(vector, image, following):
        def step(index, carry):
            x = index // ny
            y = index % ny
            made = []
            for z in range(nz):
                t = index * nz + z
                value = vector[x, y, z]
                out = image_rows(acc[t], diagonal[t], coupling[index, z : z + 1, :], value)
                made.append((out, out - SHIFT * value))
            for z, (out, rest) in enumerate(made):
                image[index * nz + z] = out
                if following is not None:
                    following[x, y, z] = rest
            return carry

        lax.fori_loop(0, nx * ny, step, 0)

    own_depth = range(1, nz + 1)
    whole = range(nz + 2)
    ext1[1:-1, 1:-1, 1:-1] = u1[...]
    split_columns(ext1, 1, ny, nx, own_depth)
    level_pass()
    pl.semaphore_wait(barrier, count + (len(across) + len(along)))
    send_rims(((u1, ext1),), rim_send.at[pl.ds(0, 1)], rim_recv.at[pl.ds(0, 1)])
    between_pass()
    await_rims(((u1, ext1),), rim_send.at[pl.ds(0, 1)], rim_recv.at[pl.ds(0, 1)])
    split_columns(ext1, 0, ny + 2, nx + 2, whole)
    rim_pass()
    finish(u1, w1, u2)

    ext2[1:-1, 1:-1, 1:-1] = u2[...]
    split_columns(ext2, 1, ny, nx, own_depth)
    send_rims(((u2, ext2),), rim_send.at[pl.ds(1, 1)], rim_recv.at[pl.ds(1, 1)])
    level_pass()
    between_pass()
    await_rims(((u2, ext2),), rim_send.at[pl.ds(1, 1)], rim_recv.at[pl.ds(1, 1)])
    split_columns(ext2, 0, ny + 2, nx + 2, whole)
    rim_pass()
    finish(u2, w2, None)

    owned = nx * ny * nz
    tile = (owned, 4, 128)
    b0, b1, b2 = (u[...].reshape(tile) for u in (u0, u1, u2))
    a0, a1, a2 = (w[...].reshape(tile) for w in (w0, w1, w2))
    wanted = [(b0, b0), (b0, b1), (b0, b2), (b0, a0), (b0, a1), (b0, a2), (b1, a1), (b1, a2), (b2, a2)]
    sums = []
    for left, right in wanted:
        both = jnp.sum(left * right, axis=0)
        sums.append(both[0:2] + both[2:4])
    stacked = jnp.concatenate(sums + [jnp.zeros((128 - 18, 128), F32)], axis=0)
    part[0] = jnp.sum(stacked.T, axis=0, keepdims=True)

    def gather(turn, peers, here, stage, width):
        made = []
        for index, peer in enumerate(peers):
            copy = pltpu.make_async_remote_copy(
                part.at[turn],
                stage.at[here],
                send_sem.at[turn, index],
                recv_sem.at[turn, index],
                device_id=peer,
                device_id_type=MESH,
            )
            copy.start()
            made.append(copy)
        stage[here] = part[turn]
        for copy in made:
            copy.wait_recv()
        total = jnp.sum(stage[...], axis=0)
        for copy in made:
            copy.wait_send()
        return total

    part[1] = gather(0, across, gy * sizes[2] + gz, plane, len(across) + 1)
    total = gather(1, along, gx, line, len(along) + 1)
    m0, m1, m2, g00, g01, g02, g11, g12, g22 = (total[:, 2 * k : 2 * k + 2] for k in range(9))
    f1 = g01 / g00
    f2 = g02 / g00
    h11 = g11 - f1 * g01
    h12 = g12 - f1 * g02
    h22 = g22 - f2 * g02
    n1 = m1 - f1 * m0
    n2 = m2 - f2 * m0
    f3 = h12 / h11
    k22 = h22 - f3 * h12
    k2 = n2 - f3 * n1
    c2 = k2 / k22
    c1 = (n1 - h12 * c2) / h11
    c0 = (m0 - g01 * c1 - g02 * c2) / g00

    def spread(c):
        pair = [jnp.broadcast_to(c[:, r : r + 1], (1, 128)) for r in range(2)]
        return jnp.concatenate(pair + pair, axis=0)[None]

    c0, c1, c2 = (spread(c) for c in (c0, c1, c2))
    answer = c0 * b0 + c1 * b1 + c2 * b2
    left = b0 - (c0 * a0 + c1 * a1 + c2 * a2)
    for t in range(32):
        for f in range(4):
            solution[f, t // 8, t % 8 : t % 8 + 1, :] = answer[t, f : f + 1]
            residual[f, t // 8, t % 8 : t % 8 + 1, :] = left[t, f : f + 1]


def on_device(positions, shield, width, hardness, softness, coupling, pair_bits, right_side):
    nx, ny, nz, lanes = hardness.shape
    owned = nx * ny * nz
    ext = (nx + 2, ny + 2, nz + 2)
    tiles = ext[0] * ext[1] * ext[2]

    def kept(value):
        return pltpu.with_memory_space_constraint(value, pltpu.VMEM)

    def far(value):
        return pltpu.with_memory_space_constraint(value, pltpu.HBM)

    def limits(size, **more):
        return pltpu.CompilerParams(vmem_limit_bytes=size, **more)

    slots = owned * 27 + 3
    param_ext, field_ext, blank = pl.pallas_call(
        first_halo,
        out_shape=(
            pltpu.VMEM(ext + (8, lanes), F32),
            pltpu.VMEM(ext + (1, lanes), F32),
            pltpu.VMEM((slots - slots % 5, 2, lanes, lanes), BF),
        ),
        in_specs=[pl.BlockSpec(memory_space=pltpu.HBM)] * 4,
        out_specs=(VMEM_SPEC,) * 3,
        scratch_shapes=[
            pltpu.VMEM((nx, ny, nz, 8, lanes), F32),
            pltpu.VMEM((nx, ny, nz, 1, lanes), F32),
            pltpu.VMEM(positions.shape, F32),
            pltpu.VMEM(shield.shape, F32),
            pltpu.VMEM(width.shape, F32),
            pltpu.VMEM(right_side.shape, F32),
            pltpu.SemaphoreType.DMA((4,)),
            pltpu.SemaphoreType.DMA((2, 26)),
            pltpu.SemaphoreType.DMA((2, 26)),
        ],
        compiler_params=limits(LIMIT, collective_id=0, has_side_effects=True),
        name="first_halo",
    )(*(far(a) for a in (positions, shield, width, right_side)))

    hard, soft, link = (a.reshape(owned // 8, 8, lanes) for a in (hardness, softness, coupling))
    store, diagonal, image0, own0, own1 = pl.pallas_call(
        build,
        out_shape=(pltpu.VMEM(blank.shape, BF),) + (pltpu.VMEM((owned, 4, lanes), F32),) * 4,
        in_specs=[SMEM_SPEC] + [VMEM_SPEC] * 6,
        input_output_aliases={6: 0},
        out_specs=(VMEM_SPEC,) * 5,
        scratch_shapes=[
            pltpu.VMEM((tiles, lanes, lanes), BF),
            pltpu.VMEM((owned, 48, 2 * lanes), BF),
            pltpu.VMEM((tiles, 16, lanes), BF),
            pltpu.VMEM((owned + 1, 16, 2 * lanes), F32),
            pltpu.SMEM((owned * 27 + GROUP,), jnp.int32),
        ],
        compiler_params=limits(LIMIT),
        name="build",
    )(
        pair_bits,
        kept(param_ext.reshape(tiles, 8, lanes)),
        kept(field_ext.reshape(tiles, 1, lanes)),
        hard,
        soft,
        link,
        kept(blank),
    )

    line = lax.axis_size("gx")
    plane = lax.axis_size("gy") * lax.axis_size("gz")
    shape = jax.ShapeDtypeStruct((4, owned // 8, 8, lanes), F32)
    answer, left = pl.pallas_call(
        solve,
        out_shape=(shape, shape),
        in_specs=[VMEM_SPEC] * 8,
        out_specs=(VMEM_SPEC, VMEM_SPEC),
        scratch_shapes=[
            pltpu.VMEM(ext + (4, lanes), F32),
            pltpu.VMEM(ext + (4, lanes), F32),
            pltpu.VMEM((nx, ny, nz, 4, lanes), F32),
            pltpu.VMEM((owned, 4, lanes), F32),
            pltpu.VMEM((owned, 4, lanes), F32),
            pltpu.VMEM((tiles, 16, lanes), BF),
            pltpu.VMEM((owned, 8, 2 * lanes), F32),
            pltpu.VMEM((2, 1, lanes), F32),
            pltpu.VMEM((plane, 1, lanes), F32),
            pltpu.VMEM((line, 1, lanes), F32),
            pltpu.SemaphoreType.DMA((2, 26)),
            pltpu.SemaphoreType.DMA((2, 26)),
            pltpu.SemaphoreType.DMA((2, plane - 1)),
            pltpu.SemaphoreType.DMA((2, plane - 1)),
        ],
        compiler_params=limits(LIMIT, collective_id=1, has_side_effects=True),
        name="solve",
    )(kept(own0), kept(own1.reshape(nx, ny, nz, 4, lanes)), kept(image0), kept(diagonal), link, kept(store),
      kept(param_ext.reshape(tiles, 8, lanes)), kept(field_ext.reshape(tiles, 1, lanes)))
    out = (4, nx, ny, nz, lanes)
    return answer.reshape(out), left.reshape(out)


def solution(mesh):
    tile = P("gx", "gy", "gz", None)
    field = P(None, "gx", "gy", "gz", None)
    return jax.shard_map(
        on_device,
        mesh=mesh,
        in_specs=(field, tile, tile, tile, tile, tile, P("gx", "gy", "gz"), field),
        out_specs=(field, field),
        check_vma=False,
    )
```

```python
import itertools

import jax
import jax.numpy as jnp
from jax import lax
from jax.experimental import pallas as pl
from jax.experimental.pallas import tpu as pltpu
from jax.sharding import PartitionSpec as P

MESH = pl.DeviceIdType.MESH
AXES = ("gx", "gy", "gz")
BF = jnp.bfloat16
F32 = jnp.float32
SHIFT = 4.0
LOG2E = 1.4426950408889634
COULOMB_GAIN = 250000.0
RESPONSE_SCALE = 0.003
GROUP = 16
LIMIT = 8800000
DIRECTIONS = [d for d in itertools.product((-1, 0, 1), repeat=3) if d != (0, 0, 0)]
VMEM_SPEC = pl.BlockSpec(memory_space=pltpu.VMEM)
SMEM_SPEC = pl.BlockSpec(memory_space=pltpu.SMEM)


def own_range(step, size):
    return pl.ds(0, size) if step == 0 else pl.ds(size - 1 if step > 0 else 0, 1)


def ghost_range(step, size):
    return pl.ds(1, size) if step == 0 else pl.ds(0 if step > 0 else size + 1, 1)


def neighbour(direction):
    exists = None
    place = []
    for axis, step in zip(AXES, direction):
        at = lax.axis_index(axis) + step
        place.append(at)
        if step:
            inside = at >= 0 if step < 0 else at < lax.axis_size(axis)
            exists = inside if exists is None else exists & inside
    return tuple(place), exists


def greet():
    barrier = pltpu.get_barrier_semaphore()
    count = jnp.int32(0)
    for direction in DIRECTIONS:
        place, exists = neighbour(direction)

        @pl.when(exists)
        def _():
            pl.semaphore_signal(barrier, inc=1, device_id=place, device_id_type=MESH)

        count = count + exists.astype(jnp.int32)
    return barrier, count


def rim_copies(pairs, index, direction, place, send_sem, recv_sem):
    made = []
    for number, (own, ext) in enumerate(pairs):
        size = own.shape[:3]
        made.append(
            pltpu.make_async_remote_copy(
                own.at[tuple(own_range(s, n) for s, n in zip(direction, size))],
                ext.at[tuple(ghost_range(s, n) for s, n in zip(direction, size))],
                send_sem.at[number, index],
                recv_sem.at[number, index],
                device_id=place,
                device_id_type=MESH,
            )
        )
    return made


def send_rims(pairs, send_sem, recv_sem):
    for index, direction in enumerate(DIRECTIONS):
        place, exists = neighbour(direction)

        @pl.when(exists)
        def _():
            for copy in rim_copies(pairs, index, direction, place, send_sem, recv_sem):
                copy.start()


def await_rims(pairs, send_sem, recv_sem):
    for index, direction in enumerate(DIRECTIONS):
        place, exists = neighbour(direction)
        source, incoming = neighbour(tuple(-s for s in direction))

        @pl.when(incoming)
        def _():
            for copy in rim_copies(pairs, index, direction, place, send_sem, recv_sem):
                copy.wait_recv()

        @pl.when(exists)
        def _():
            for copy in rim_copies(pairs, index, direction, place, send_sem, recv_sem):
                copy.wait_send()


def first_halo(pos_in, shield_in, width_in, rhs_in, param_ext, field_ext, store, *scratch):
    param_own, last_own, pos, shield, width, rhs, load_sem, send_sem, recv_sem = scratch
    loads = [
        pltpu.make_async_copy(source, target, load_sem.at[index])
        for index, (source, target) in enumerate(
            ((pos_in, pos), (shield_in, shield), (width_in, width), (rhs_in, rhs))
        )
    ]
    for load in loads:
        load.start()
    param_ext[...] = jnp.zeros_like(param_ext)
    field_ext[...] = jnp.zeros_like(field_ext)
    barrier, count = greet()
    for load in loads:
        load.wait()
    nx, ny, nz = param_own.shape[:3]
    for x in range(nx):
        for y in range(ny):
            columns = [pos[0, x, y], pos[1, x, y], pos[2, x, y], shield[x, y], width[x, y]]
            columns = columns + [rhs[f, x, y] for f in range(4)]
            for z in range(nz):
                for f in range(9):
                    row = columns[f][z : z + 1]
                    if f < 8:
                        param_own[x, y, z, f : f + 1, :] = row
                        param_ext[x + 1, y + 1, z + 1, f : f + 1, :] = row
                    else:
                        last_own[x, y, z] = row
                        field_ext[x + 1, y + 1, z + 1] = row
    pl.semaphore_wait(barrier, count)
    pairs = ((param_own, param_ext), (last_own, field_ext))
    send_rims(pairs, send_sem, recv_sem)
    slots = store.shape[0]

    def clear(index, carry):
        store[pl.ds(index * 5, 5)] = jnp.zeros((5,) + store.shape[1:], BF)
        return carry

    lax.fori_loop(0, slots // 5, clear, 0)
    await_rims(pairs, send_sem, recv_sem)


def split3(value):
    first = value.astype(BF)
    rest = value - first.astype(F32)
    second = rest.astype(BF)
    third = (rest - second.astype(F32)).astype(BF)
    return first.astype(F32), second.astype(F32), third.astype(F32)


def rows_of(pieces):
    row = lax.broadcasted_iota(jnp.int32, (8, 128), 0)
    value = jnp.zeros((8, 128), F32)
    for index, piece in pieces:
        value = jnp.where(row == index, piece, value)
    return value


def centred(param, ex, ey, ez, half):
    row = lax.broadcasted_iota(jnp.int32, (8, 128), 0)
    offset = jnp.where(row == 0, ex, jnp.where(row == 1, ey, ez)).astype(F32) - jnp.where(
        row == 0, half[0], jnp.where(row == 1, half[1], half[2])
    )
    place = param + offset
    square = jnp.sum(jnp.where(row < 3, place * place, 0.0), axis=0, keepdims=True)
    return row, place, jnp.broadcast_to(square, (8, 128))


def partner_features(param, ex, ey, ez, half):
    row, place, square = centred(param, ex, ey, ez, half)
    value = jnp.where(row < 3, place, jnp.where(row == 3, param, 0.0))
    value = jnp.where(row == 4, square, jnp.where(row == 5, 1.0, value))
    one, two, three = split3(value)
    return jnp.concatenate([one, two, one, two, three, one], axis=0)


def own_features(param, ex, ey, ez, half):
    row, place, square = centred(param, ex, ey, ez, half)
    sides = []
    for gain, shielded in ((-LOG2E, 0.0), (COULOMB_GAIN, COULOMB_GAIN)):
        value = jnp.where(row < 3, (-2.0 * gain) * place, jnp.where(row == 3, shielded * param, 0.0))
        value = jnp.where(row == 4, gain, jnp.where(row == 5, gain * square, value))
        one, two, three = split3(value)
        sides.append(jnp.concatenate([one, one, two, two, one, three], axis=0))
    return jnp.concatenate(sides, axis=1)


def split_fields(load, halves, tiles):
    ones = jnp.ones((8, 128), F32)

    def step(index, carry):
        values = [load(index * 16 + sub) for sub in range(16)]
        parts = []
        for value in values:
            high = value.astype(BF).astype(F32)
            parts.append(jnp.concatenate([high, value - high, ones], axis=0).astype(BF))
        for sub in range(16):
            halves[index * 16 + sub] = parts[sub]
        return carry

    lax.fori_loop(0, tiles // 16, step, 0)


def apply_group(base, size, entries, halves, store, acc, recent=False):
    for sub in range(size):
        code = entries[base + sub]
        e = code & 255
        t = lax.shift_right_logical(code, 14) & 63
        slot = sub if recent else lax.shift_right_logical(code, 20)
        both = jnp.concatenate([store[slot, 0], store[slot, 1]], axis=1)
        acc[t] = acc[t] + jnp.dot(halves[e], both, preferred_element_type=F32)


def image_rows(out, diagonal, link, value):
    row = lax.broadcasted_iota(jnp.int32, (4, 128), 0)
    summed = out[0:4] + out[4:8]
    pair = jnp.where(row < 2, summed[:, :128], -summed[:, 128:])
    swapped = jnp.concatenate([value[2:4], value[0:2]], axis=0)
    return diagonal * value + pair + link * swapped


def finish_all(owned, make):
    def step(index, carry):
        results = [make(index, sub) for sub in range(8)]
        for sub, (targets, values) in enumerate(results):
            for target, value in zip(targets, values):
                target[index * 8 + sub] = value
        return carry

    lax.fori_loop(0, owned // 8, step, 0)


def build(
    bits, param, field, hardness, softness, coupling, blank, store, diagonal, image, own, send,
    features, mine, halves, acc, entries, recent
):
    ey_size, ez_size = 4, 10
    half = (2.0, 2.0, 5.0)
    tiles = 160
    owned = 32

    def place_of(t):
        return ((t // 16 + 1) * ey_size + t // 8 % 2 + 1) * ez_size + t % 8 + 1

    def features_step(index, at):
        ex = lax.shift_right_logical(index, 2)
        ey = index & 3
        loaded = [param[index * ez_size + ez] for ez in range(ez_size)]
        made = [partner_features(loaded[ez], ex, ey, ez, half).T.astype(BF) for ez in range(ez_size)]
        for ez in range(ez_size):
            features[index * ez_size + ez, :, 0:48] = made[ez]
        for sub in range(2):
            t = index * 2 + sub
            x = lax.shift_right_logical(t, 4)
            y = lax.shift_right_logical(t, 3) & 1
            z = t & 7
            word = bits[x, y, z]
            own_code = ((x + 1) * ey_size + y + 1) * ez_size + z + 1 + 256 * t + 16384 * t + (27 << 20) * t
            entries[t] = own_code + (13 << 20)
            for code in range(27):
                if code == 13:
                    continue
                shift = ((code // 9 - 1) * ey_size + (code // 3 % 3 - 1)) * ez_size + code % 3 - 1
                entries[at] = own_code + shift + (code << 20)
                at = at + (lax.shift_right_logical(word, code) & 1)
        return at

    total = lax.fori_loop(0, 16, features_step, jnp.int32(owned))
    middle = (ey_size + 1) * ez_size + 1
    for sub in range(GROUP):
        entries[total + sub] = middle + 16384 * owned + ((27 * owned) << 20)

    def own_step(index, carry):
        ex = lax.shift_right_logical(index, 1) + 1
        ey = (index & 1) + 1
        first = (ex * ey_size + ey) * ez_size + 1
        made = [own_features(param[first + z], ex, ey, z + 1, half).astype(BF) for z in range(8)]
        for z in range(8):
            mine[index * 8 + z] = made[z]
        return carry

    lax.fori_loop(0, owned // 8, own_step, 0)
    split_fields(lambda e: jnp.concatenate([param[e, 5:8, :], field[e]], axis=0), halves, tiles)
    acc[...] = jnp.zeros_like(acc)

    def pair(position, sub, masked):
        code = entries[position]
        e = code & 255
        t = lax.shift_right_logical(code, 8) & 63
        slot = lax.shift_right_logical(code, 20)
        both = jnp.dot(features[e, :, 0:48], mine[t], preferred_element_type=F32)
        partner_width = jnp.broadcast_to(param[e, 4:5, :], (128, 128)).T
        widths = partner_width + param[place_of(t), 4:5, :]
        coulomb = lax.rsqrt(both[:, 128:])
        response = RESPONSE_SCALE * jnp.exp2(both[:, :128] / widths)
        if masked:
            same = lax.broadcasted_iota(jnp.int32, (128, 128), 0) == lax.broadcasted_iota(
                jnp.int32, (128, 128), 1
            )
            coulomb = jnp.where(same, 0.0, coulomb.astype(F32))
            response = jnp.where(same, 0.0, response.astype(F32))
        for side, value in enumerate((coulomb.astype(BF), response.astype(BF))):
            recent[sub, side] = value
            store[slot, side] = value

    def self_step(index, carry):
        for sub in range(GROUP):
            pair(index * GROUP + sub, sub, True)
        return carry

    lax.fori_loop(0, owned // GROUP, self_step, 0)
    apply_group(0, owned - GROUP, entries, halves, store, acc)

    def pair_step(index, carry):
        base = owned + index * GROUP
        for sub in range(GROUP):
            apply_group(base - GROUP + sub, 1, entries, halves, recent.at[pl.ds(sub, 1)], acc, True)
            pair(base + sub, sub, False)
        return carry

    groups = (total - owned + GROUP - 1) // GROUP
    lax.fori_loop(0, groups, pair_step, 0)
    last = owned + (groups - 1) * GROUP
    apply_group(last, GROUP, entries, halves, recent, acc, True)
    row = lax.broadcasted_iota(jnp.int32, (4, 128), 0)

    def make(index, sub):
        out = acc[index * 8 + sub]
        e = place_of(index * 8) + sub
        value = jnp.concatenate([param[e, 5:8, :], field[e]], axis=0)
        top = hardness[index, sub : sub + 1, :] + out[8:9, :128]
        low = softness[index, sub : sub + 1, :] + out[8:9, 128:]
        diag = jnp.where(row < 2, top, low)
        made = image_rows(out, diag, coupling[index, sub : sub + 1, :], value)
        return (diagonal, image, own, send), (diag, made, value, made - SHIFT * value)

    finish_all(owned, make)


INSIDE = {0: (0, 1), 1: (-1, 0)}
FLAT = list(itertools.product((-1, 0, 1), repeat=2))


def solve(u0, u1, w0, diagonal, coupling, store, unused, idle, solution, residual, *scratch):
    ext1, ext2, u2, w1, w2, halves, acc, part, plane, line, rim_send, rim_recv, send_sem, recv_sem = scratch
    nx, ny, nz = u1.shape[:3]
    ey_size, ez_size = ny + 2, nz + 2
    sizes = [lax.axis_size(axis) for axis in AXES]
    gx, gy, gz = (lax.axis_index(axis) for axis in AXES)
    across = []
    for a in range(sizes[1]):
        for b in range(sizes[2]):
            if a or b:
                across.append((gx, lax.rem(gy + a, sizes[1]), lax.rem(gz + b, sizes[2])))
    along = [(lax.rem(gx + a, sizes[0]), gy, gz) for a in range(1, sizes[0])]
    ext1[...] = jnp.zeros_like(ext1)
    ext2[...] = jnp.zeros_like(ext2)
    barrier, count = greet()
    for peer in across + along:
        pl.semaphore_signal(barrier, inc=1, device_id=peer, device_id_type=MESH)

    def split_columns(ext, lowest, columns, rows, depth):
        def step(index, carry):
            x = index // columns + lowest
            y = index % columns + lowest
            values = [ext[x, y, z] for z in depth]
            parts = []
            for value in values:
                high = value.astype(BF).astype(F32)
                parts.append(jnp.concatenate([high, value - high, jnp.zeros((8, 128), F32)], axis=0).astype(BF))
            for z, made in zip(depth, parts):
                halves[(x * ey_size + y) * ez_size + z] = made
            return carry

        lax.fori_loop(0, columns * rows, step, 0)

    def tile_sum(x, y, z, offsets):
        total = None
        for dx, dy, dz in offsets:
            slot = ((x * ny + y) * nz + z) * 27 + (dx + 1) * 9 + (dy + 1) * 3 + dz + 1
            e = ((x + 1 + dx) * ey_size + y + 1 + dy) * ez_size + z + 1 + dz
            both = jnp.concatenate([store[slot, 0], store[slot, 1]], axis=1)
            out = jnp.dot(halves[e], both, preferred_element_type=F32)
            total = out if total is None else total + out
        return total[:8]

    columns = [(x, y) for x in range(nx) for y in range(ny)]

    def inside(x, y):
        return [(dx, dy) for dx in INSIDE[x] for dy in INSIDE[y]]

    def outside(x, y):
        return [d for d in FLAT if d not in inside(x, y)]

    def level_pass():
        def step(index, carry):
            for sub in range(2):
                z = index * 2 + sub
                for x, y in columns:
                    acc[(x * ny + y) * nz + z] = tile_sum(x, y, z, [d + (0,) for d in inside(x, y)])
            return carry

        lax.fori_loop(0, nz // 2, step, 0)

    def between_pass():
        def step(z, carry):
            for x, y in columns:
                t = (x * ny + y) * nz + z
                acc[t] = acc[t] + tile_sum(x, y, z, [d + (1,) for d in inside(x, y)])
                acc[t + 1] = acc[t + 1] + tile_sum(x, y, z + 1, [d + (-1,) for d in inside(x, y)])
            return carry

        lax.fori_loop(0, nz - 1, step, 0)

    def rim_pass():
        for x, y in columns:
            for z, dz in ((0, -1), (nz - 1, 1)):
                t = (x * ny + y) * nz + z
                acc[t] = acc[t] + tile_sum(x, y, z, [d + (dz,) for d in inside(x, y)])

        def step(index, carry):
            for sub in range(2):
                z = index * 2 + sub
                for x, y in columns:
                    t = (x * ny + y) * nz + z
                    around = [d + (dz,) for d in outside(x, y) for dz in (-1, 0, 1)]
                    acc[t] = acc[t] + tile_sum(x, y, z, around)
            return carry

        lax.fori_loop(0, nz // 2, step, 0)

    def finish(vector, image, following):
        def step(index, carry):
            x = index // ny
            y = index % ny
            made = []
            for z in range(nz):
                t = index * nz + z
                value = vector[x, y, z]
                out = image_rows(acc[t], diagonal[t], coupling[index, z : z + 1, :], value)
                made.append((out, out - SHIFT * value))
            for z, (out, rest) in enumerate(made):
                image[index * nz + z] = out
                if following is not None:
                    following[x, y, z] = rest
            return carry

        lax.fori_loop(0, nx * ny, step, 0)

    own_depth = range(1, nz + 1)
    whole = range(nz + 2)
    ext1[1:-1, 1:-1, 1:-1] = u1[...]
    split_columns(ext1, 1, ny, nx, own_depth)
    level_pass()
    pl.semaphore_wait(barrier, count + (len(across) + len(along)))
    send_rims(((u1, ext1),), rim_send.at[pl.ds(0, 1)], rim_recv.at[pl.ds(0, 1)])
    between_pass()
    await_rims(((u1, ext1),), rim_send.at[pl.ds(0, 1)], rim_recv.at[pl.ds(0, 1)])
    split_columns(ext1, 0, ny + 2, nx + 2, whole)
    rim_pass()
    finish(u1, w1, u2)

    ext2[1:-1, 1:-1, 1:-1] = u2[...]
    split_columns(ext2, 1, ny, nx, own_depth)
    send_rims(((u2, ext2),), rim_send.at[pl.ds(1, 1)], rim_recv.at[pl.ds(1, 1)])
    level_pass()
    between_pass()
    await_rims(((u2, ext2),), rim_send.at[pl.ds(1, 1)], rim_recv.at[pl.ds(1, 1)])
    split_columns(ext2, 0, ny + 2, nx + 2, whole)
    rim_pass()
    finish(u2, w2, None)

    owned = nx * ny * nz
    tile = (owned, 4, 128)
    b0, b1, b2 = (u[...].reshape(tile) for u in (u0, u1, u2))
    a0, a1, a2 = (w[...].reshape(tile) for w in (w0, w1, w2))
    wanted = [(b0, b0), (b0, b1), (b0, b2), (b0, a0), (b0, a1), (b0, a2), (b1, a1), (b1, a2), (b2, a2)]
    sums = []
    for left, right in wanted:
        both = jnp.sum(left * right, axis=0)
        sums.append(both[0:2] + both[2:4])
    stacked = jnp.concatenate(sums + [jnp.zeros((128 - 18, 128), F32)], axis=0)
    part[0] = jnp.sum(stacked.T, axis=0, keepdims=True)

    def gather(turn, peers, here, stage, width):
        made = []
        for index, peer in enumerate(peers):
            copy = pltpu.make_async_remote_copy(
                part.at[turn],
                stage.at[here],
                send_sem.at[turn, index],
                recv_sem.at[turn, index],
                device_id=peer,
                device_id_type=MESH,
            )
            copy.start()
            made.append(copy)
        stage[here] = part[turn]
        for copy in made:
            copy.wait_recv()
        total = jnp.sum(stage[...], axis=0)
        for copy in made:
            copy.wait_send()
        return total

    part[1] = gather(0, across, gy * sizes[2] + gz, plane, len(across) + 1)
    total = gather(1, along, gx, line, len(along) + 1)
    m0, m1, m2, g00, g01, g02, g11, g12, g22 = (total[:, 2 * k : 2 * k + 2] for k in range(9))
    f1 = g01 / g00
    f2 = g02 / g00
    h11 = g11 - f1 * g01
    h12 = g12 - f1 * g02
    h22 = g22 - f2 * g02
    n1 = m1 - f1 * m0
    n2 = m2 - f2 * m0
    f3 = h12 / h11
    k22 = h22 - f3 * h12
    k2 = n2 - f3 * n1
    c2 = k2 / k22
    c1 = (n1 - h12 * c2) / h11
    c0 = (m0 - g01 * c1 - g02 * c2) / g00

    def spread(c):
        pair = [jnp.broadcast_to(c[:, r : r + 1], (1, 128)) for r in range(2)]
        return jnp.concatenate(pair + pair, axis=0)[None]

    c0, c1, c2 = (spread(c) for c in (c0, c1, c2))
    answer = c0 * b0 + c1 * b1 + c2 * b2
    left = b0 - (c0 * a0 + c1 * a1 + c2 * a2)
    for t in range(32):
        for f in range(4):
            solution[f, t // 8, t % 8 : t % 8 + 1, :] = answer[t, f : f + 1]
            residual[f, t // 8, t % 8 : t % 8 + 1, :] = left[t, f : f + 1]


def on_device(positions, shield, width, hardness, softness, coupling, pair_bits, right_side):
    nx, ny, nz, lanes = hardness.shape
    owned = nx * ny * nz
    ext = (nx + 2, ny + 2, nz + 2)
    tiles = ext[0] * ext[1] * ext[2]

    def kept(value):
        return pltpu.with_memory_space_constraint(value, pltpu.VMEM)

    def far(value):
        return pltpu.with_memory_space_constraint(value, pltpu.HBM)

    def limits(size, **more):
        return pltpu.CompilerParams(vmem_limit_bytes=size, **more)

    slots = owned * 27 + 3
    param_ext, field_ext, blank = pl.pallas_call(
        first_halo,
        out_shape=(
            pltpu.VMEM(ext + (8, lanes), F32),
            pltpu.VMEM(ext + (1, lanes), F32),
            pltpu.VMEM((slots - slots % 5, 2, lanes, lanes), BF),
        ),
        in_specs=[pl.BlockSpec(memory_space=pltpu.HBM)] * 4,
        out_specs=(VMEM_SPEC,) * 3,
        scratch_shapes=[
            pltpu.VMEM((nx, ny, nz, 8, lanes), F32),
            pltpu.VMEM((nx, ny, nz, 1, lanes), F32),
            pltpu.VMEM(positions.shape, F32),
            pltpu.VMEM(shield.shape, F32),
            pltpu.VMEM(width.shape, F32),
            pltpu.VMEM(right_side.shape, F32),
            pltpu.SemaphoreType.DMA((4,)),
            pltpu.SemaphoreType.DMA((2, 26)),
            pltpu.SemaphoreType.DMA((2, 26)),
        ],
        compiler_params=limits(LIMIT, collective_id=0, has_side_effects=True),
        name="first_halo",
    )(*(far(a) for a in (positions, shield, width, right_side)))

    hard, soft, link = (a.reshape(owned // 8, 8, lanes) for a in (hardness, softness, coupling))
    store, diagonal, image0, own0, own1 = pl.pallas_call(
        build,
        out_shape=(pltpu.VMEM(blank.shape, BF),) + (pltpu.VMEM((owned, 4, lanes), F32),) * 4,
        in_specs=[SMEM_SPEC] + [VMEM_SPEC] * 6,
        input_output_aliases={6: 0},
        out_specs=(VMEM_SPEC,) * 5,
        scratch_shapes=[
            pltpu.VMEM((tiles, lanes, lanes), BF),
            pltpu.VMEM((owned, 48, 2 * lanes), BF),
            pltpu.VMEM((tiles, 16, lanes), BF),
            pltpu.VMEM((owned + 1, 16, 2 * lanes), F32),
            pltpu.SMEM((owned * 27 + GROUP,), jnp.int32),
            pltpu.VMEM((GROUP, 2, lanes, lanes), BF),
        ],
        compiler_params=limits(LIMIT),
        name="build",
    )(
        pair_bits,
        kept(param_ext.reshape(tiles, 8, lanes)),
        kept(field_ext.reshape(tiles, 1, lanes)),
        hard,
        soft,
        link,
        kept(blank),
    )

    line = lax.axis_size("gx")
    plane = lax.axis_size("gy") * lax.axis_size("gz")
    shape = pltpu.VMEM((4, owned // 8, 8, lanes), F32)
    answer, left = pl.pallas_call(
        solve,
        out_shape=(shape, shape),
        in_specs=[VMEM_SPEC] * 8,
        out_specs=(VMEM_SPEC, VMEM_SPEC),
        scratch_shapes=[
            pltpu.VMEM(ext + (4, lanes), F32),
            pltpu.VMEM(ext + (4, lanes), F32),
            pltpu.VMEM((nx, ny, nz, 4, lanes), F32),
            pltpu.VMEM((owned, 4, lanes), F32),
            pltpu.VMEM((owned, 4, lanes), F32),
            pltpu.VMEM((tiles, 16, lanes), BF),
            pltpu.VMEM((owned, 8, 2 * lanes), F32),
            pltpu.VMEM((2, 1, lanes), F32),
            pltpu.VMEM((plane, 1, lanes), F32),
            pltpu.VMEM((line, 1, lanes), F32),
            pltpu.SemaphoreType.DMA((2, 26)),
            pltpu.SemaphoreType.DMA((2, 26)),
            pltpu.SemaphoreType.DMA((2, plane - 1)),
            pltpu.SemaphoreType.DMA((2, plane - 1)),
        ],
        compiler_params=limits(LIMIT, collective_id=1, has_side_effects=True),
        name="solve",
    )(kept(own0), kept(own1.reshape(nx, ny, nz, 4, lanes)), kept(image0), kept(diagonal), link, kept(store),
      kept(param_ext.reshape(tiles, 8, lanes)), kept(field_ext.reshape(tiles, 1, lanes)))
    out = (4, nx, ny, nz, lanes)
    return answer.reshape(out), left.reshape(out)


def solution(mesh):
    tile = P("gx", "gy", "gz", None)
    field = P(None, "gx", "gy", "gz", None)
    return jax.shard_map(
        on_device,
        mesh=mesh,
        in_specs=(field, tile, tile, tile, tile, tile, P("gx", "gy", "gz"), field),
        out_specs=(field, field),
        check_vma=False,
    )
```

```python
import itertools

import jax
import jax.numpy as jnp
from jax import lax
from jax.experimental import pallas as pl
from jax.experimental.pallas import tpu as pltpu
from jax.sharding import PartitionSpec as P

MESH = pl.DeviceIdType.MESH
AXES = ("gx", "gy", "gz")
BF = jnp.bfloat16
F32 = jnp.float32
SHIFT = 4.0
LOG2E = 1.4426950408889634
COULOMB_GAIN = 250000.0
RESPONSE_SCALE = 0.003
GROUP = 16
LIMIT = 8800000
DIRECTIONS = [d for d in itertools.product((-1, 0, 1), repeat=3) if d != (0, 0, 0)]
VMEM_SPEC = pl.BlockSpec(memory_space=pltpu.VMEM)
SMEM_SPEC = pl.BlockSpec(memory_space=pltpu.SMEM)


def own_range(step, size):
    return pl.ds(0, size) if step == 0 else pl.ds(size - 1 if step > 0 else 0, 1)


def ghost_range(step, size):
    return pl.ds(1, size) if step == 0 else pl.ds(0 if step > 0 else size + 1, 1)


def neighbour(direction):
    exists = None
    place = []
    for axis, step in zip(AXES, direction):
        at = lax.axis_index(axis) + step
        place.append(at)
        if step:
            inside = at >= 0 if step < 0 else at < lax.axis_size(axis)
            exists = inside if exists is None else exists & inside
    return tuple(place), exists


def greet():
    barrier = pltpu.get_barrier_semaphore()
    count = jnp.int32(0)
    for direction in DIRECTIONS:
        place, exists = neighbour(direction)

        @pl.when(exists)
        def _():
            pl.semaphore_signal(barrier, inc=1, device_id=place, device_id_type=MESH)

        count = count + exists.astype(jnp.int32)
    return barrier, count


def rim_copies(pairs, index, direction, place, send_sem, recv_sem):
    made = []
    for number, (own, ext) in enumerate(pairs):
        size = own.shape[:3]
        made.append(
            pltpu.make_async_remote_copy(
                own.at[tuple(own_range(s, n) for s, n in zip(direction, size))],
                ext.at[tuple(ghost_range(s, n) for s, n in zip(direction, size))],
                send_sem.at[number, index],
                recv_sem.at[number, index],
                device_id=place,
                device_id_type=MESH,
            )
        )
    return made


def send_rims(pairs, send_sem, recv_sem):
    for index, direction in enumerate(DIRECTIONS):
        place, exists = neighbour(direction)

        @pl.when(exists)
        def _():
            for copy in rim_copies(pairs, index, direction, place, send_sem, recv_sem):
                copy.start()


def await_rims(pairs, send_sem, recv_sem):
    for index, direction in enumerate(DIRECTIONS):
        place, exists = neighbour(direction)
        source, incoming = neighbour(tuple(-s for s in direction))

        @pl.when(incoming)
        def _():
            for copy in rim_copies(pairs, index, direction, place, send_sem, recv_sem):
                copy.wait_recv()

        @pl.when(exists)
        def _():
            for copy in rim_copies(pairs, index, direction, place, send_sem, recv_sem):
                copy.wait_send()


def first_halo(pos_in, shield_in, width_in, rhs_in, param_ext, field_ext, store, *scratch):
    param_own, last_own, empty, pos, shield, width, rhs, load_sem, send_sem, recv_sem = scratch
    loads = [
        pltpu.make_async_copy(source, target, load_sem.at[index])
        for index, (source, target) in enumerate(
            ((pos_in, pos), (shield_in, shield), (width_in, width), (rhs_in, rhs))
        )
    ]
    for load in loads:
        load.start()
    param_ext[...] = jnp.zeros_like(param_ext)
    field_ext[...] = jnp.zeros_like(field_ext)
    empty[...] = jnp.zeros_like(empty)
    barrier, count = greet()
    for load in loads:
        load.wait()
    nx, ny, nz = param_own.shape[:3]
    for x in range(nx):
        for y in range(ny):
            columns = [pos[0, x, y], pos[1, x, y], pos[2, x, y], shield[x, y], width[x, y]]
            columns = columns + [rhs[f, x, y] for f in range(4)]
            for z in range(nz):
                for f in range(9):
                    row = columns[f][z : z + 1]
                    if f < 8:
                        param_own[x, y, z, f : f + 1, :] = row
                        param_ext[x + 1, y + 1, z + 1, f : f + 1, :] = row
                    else:
                        last_own[x, y, z] = row
                        field_ext[x + 1, y + 1, z + 1] = row
    pl.semaphore_wait(barrier, count)
    pairs = ((param_own, param_ext), (last_own, field_ext))
    send_rims(pairs, send_sem, recv_sem)
    slots = store.shape[0]

    def clear(index, carry):
        nothing = empty[...].astype(BF)
        for sub in range(5):
            for side in range(2):
                store[index * 5 + sub, side] = nothing
        return carry

    lax.fori_loop(0, slots // 5, clear, 0)
    await_rims(pairs, send_sem, recv_sem)


def split3(value):
    first = value.astype(BF)
    rest = value - first.astype(F32)
    second = rest.astype(BF)
    third = (rest - second.astype(F32)).astype(BF)
    return first.astype(F32), second.astype(F32), third.astype(F32)


def rows_of(pieces):
    row = lax.broadcasted_iota(jnp.int32, (8, 128), 0)
    value = jnp.zeros((8, 128), F32)
    for index, piece in pieces:
        value = jnp.where(row == index, piece, value)
    return value


def centred(param, ex, ey, ez, half):
    row = lax.broadcasted_iota(jnp.int32, (8, 128), 0)
    offset = jnp.where(row == 0, ex, jnp.where(row == 1, ey, ez)).astype(F32) - jnp.where(
        row == 0, half[0], jnp.where(row == 1, half[1], half[2])
    )
    place = param + offset
    square = jnp.sum(jnp.where(row < 3, place * place, 0.0), axis=0, keepdims=True)
    return row, place, jnp.broadcast_to(square, (8, 128))


def partner_features(param, ex, ey, ez, half):
    row, place, square = centred(param, ex, ey, ez, half)
    value = jnp.where(row < 3, place, jnp.where(row == 3, param, 0.0))
    value = jnp.where(row == 4, square, jnp.where(row == 5, 1.0, value))
    one, two, three = split3(value)
    return jnp.concatenate([one, two, one, two, three, one], axis=0)


def own_features(param, ex, ey, ez, half):
    row, place, square = centred(param, ex, ey, ez, half)
    sides = []
    for gain, shielded in ((-LOG2E, 0.0), (COULOMB_GAIN, COULOMB_GAIN)):
        value = jnp.where(row < 3, (-2.0 * gain) * place, jnp.where(row == 3, shielded * param, 0.0))
        value = jnp.where(row == 4, gain, jnp.where(row == 5, gain * square, value))
        one, two, three = split3(value)
        sides.append(jnp.concatenate([one, one, two, two, one, three], axis=0))
    return jnp.concatenate(sides, axis=1)


def split_fields(load, halves, tiles):
    ones = jnp.ones((8, 128), F32)

    def step(index, carry):
        values = [load(index * 16 + sub) for sub in range(16)]
        parts = []
        for value in values:
            high = value.astype(BF).astype(F32)
            parts.append(jnp.concatenate([high, value - high, ones], axis=0).astype(BF))
        for sub in range(16):
            halves[index * 16 + sub] = parts[sub]
        return carry

    lax.fori_loop(0, tiles // 16, step, 0)


def apply_group(base, size, entries, halves, store, acc, recent=False):
    for sub in range(size):
        code = entries[base + sub]
        e = code & 255
        t = lax.shift_right_logical(code, 14) & 63
        slot = sub if recent else lax.shift_right_logical(code, 20)
        both = jnp.concatenate([store[slot, 0], store[slot, 1]], axis=1)
        acc[t] = acc[t] + jnp.dot(halves[e], both, preferred_element_type=F32)


def image_rows(out, diagonal, link, value):
    row = lax.broadcasted_iota(jnp.int32, (4, 128), 0)
    summed = out[0:4] + out[4:8]
    pair = jnp.where(row < 2, summed[:, :128], -summed[:, 128:])
    swapped = jnp.concatenate([value[2:4], value[0:2]], axis=0)
    return diagonal * value + pair + link * swapped


def finish_all(owned, make):
    def step(index, carry):
        results = [make(index, sub) for sub in range(8)]
        for sub, (targets, values) in enumerate(results):
            for target, value in zip(targets, values):
                target[index * 8 + sub] = value
        return carry

    lax.fori_loop(0, owned // 8, step, 0)


def build(
    bits, param, field, hardness, softness, coupling, blank, store, diagonal, image, own, send,
    features, mine, halves, acc, entries, recent
):
    ey_size, ez_size = 4, 10
    half = (2.0, 2.0, 5.0)
    tiles = 160
    owned = 32

    def place_of(t):
        return ((t // 16 + 1) * ey_size + t // 8 % 2 + 1) * ez_size + t % 8 + 1

    def features_step(index, at):
        ex = lax.shift_right_logical(index, 2)
        ey = index & 3
        loaded = [param[index * ez_size + ez] for ez in range(ez_size)]
        made = [partner_features(loaded[ez], ex, ey, ez, half).T.astype(BF) for ez in range(ez_size)]
        for ez in range(ez_size):
            features[index * ez_size + ez, :, 0:48] = made[ez]
        for sub in range(2):
            t = index * 2 + sub
            x = lax.shift_right_logical(t, 4)
            y = lax.shift_right_logical(t, 3) & 1
            z = t & 7
            word = bits[x, y, z]
            own_code = ((x + 1) * ey_size + y + 1) * ez_size + z + 1 + 256 * t + 16384 * t + (27 << 20) * t
            entries[t] = own_code + (13 << 20)
            for code in range(27):
                if code == 13:
                    continue
                shift = ((code // 9 - 1) * ey_size + (code // 3 % 3 - 1)) * ez_size + code % 3 - 1
                entries[at] = own_code + shift + (code << 20)
                at = at + (lax.shift_right_logical(word, code) & 1)
        return at

    total = lax.fori_loop(0, 16, features_step, jnp.int32(owned))
    middle = (ey_size + 1) * ez_size + 1
    for sub in range(GROUP):
        entries[total + sub] = middle + 16384 * owned + ((27 * owned) << 20)

    def own_step(index, carry):
        ex = lax.shift_right_logical(index, 1) + 1
        ey = (index & 1) + 1
        first = (ex * ey_size + ey) * ez_size + 1
        made = [own_features(param[first + z], ex, ey, z + 1, half).astype(BF) for z in range(8)]
        for z in range(8):
            mine[index * 8 + z] = made[z]
        return carry

    lax.fori_loop(0, owned // 8, own_step, 0)
    split_fields(lambda e: jnp.concatenate([param[e, 5:8, :], field[e]], axis=0), halves, tiles)
    acc[...] = jnp.zeros_like(acc)

    def pair(position, sub, masked):
        code = entries[position]
        e = code & 255
        t = lax.shift_right_logical(code, 8) & 63
        slot = lax.shift_right_logical(code, 20)
        both = jnp.dot(features[e, :, 0:48], mine[t], preferred_element_type=F32)
        partner_width = jnp.broadcast_to(param[e, 4:5, :], (128, 128)).T
        widths = partner_width + param[place_of(t), 4:5, :]
        coulomb = lax.rsqrt(both[:, 128:].astype(BF))
        response = RESPONSE_SCALE * jnp.exp2(both[:, :128] / widths)
        if masked:
            same = lax.broadcasted_iota(jnp.int32, (128, 128), 0) == lax.broadcasted_iota(
                jnp.int32, (128, 128), 1
            )
            coulomb = jnp.where(same, 0.0, coulomb.astype(F32))
            response = jnp.where(same, 0.0, response.astype(F32))
        for side, value in enumerate((coulomb.astype(BF), response.astype(BF))):
            recent[sub, side] = value
            store[slot, side] = value

    def self_step(index, carry):
        for sub in range(GROUP):
            pair(index * GROUP + sub, sub, True)
        return carry

    lax.fori_loop(0, owned // GROUP, self_step, 0)
    apply_group(0, owned - GROUP, entries, halves, store, acc)

    def pair_step(index, carry):
        base = owned + index * GROUP
        for sub in range(GROUP):
            apply_group(base - GROUP + sub, 1, entries, halves, recent.at[pl.ds(sub, 1)], acc, True)
            pair(base + sub, sub, False)
        return carry

    groups = (total - owned + GROUP - 1) // GROUP
    lax.fori_loop(0, groups, pair_step, 0)
    last = owned + (groups - 1) * GROUP
    apply_group(last, GROUP, entries, halves, recent, acc, True)
    row = lax.broadcasted_iota(jnp.int32, (4, 128), 0)

    def make(index, sub):
        out = acc[index * 8 + sub]
        e = place_of(index * 8) + sub
        value = jnp.concatenate([param[e, 5:8, :], field[e]], axis=0)
        top = hardness[index, sub : sub + 1, :] + out[8:9, :128]
        low = softness[index, sub : sub + 1, :] + out[8:9, 128:]
        diag = jnp.where(row < 2, top, low)
        made = image_rows(out, diag, coupling[index, sub : sub + 1, :], value)
        return (diagonal, image, own, send), (diag, made, value, made - SHIFT * value)

    finish_all(owned, make)


INSIDE = {0: (0, 1), 1: (-1, 0)}
FLAT = list(itertools.product((-1, 0, 1), repeat=2))


def solve(u0, u1, w0, diagonal, coupling, store, unused, idle, solution, residual, *scratch):
    ext1, ext2, u2, w1, w2, halves, acc, part, plane, line, rim_send, rim_recv, send_sem, recv_sem = scratch
    nx, ny, nz = u1.shape[:3]
    ey_size, ez_size = ny + 2, nz + 2
    sizes = [lax.axis_size(axis) for axis in AXES]
    gx, gy, gz = (lax.axis_index(axis) for axis in AXES)
    across = []
    for a in range(sizes[1]):
        for b in range(sizes[2]):
            if a or b:
                across.append((gx, lax.rem(gy + a, sizes[1]), lax.rem(gz + b, sizes[2])))
    along = [(lax.rem(gx + a, sizes[0]), gy, gz) for a in range(1, sizes[0])]
    ext1[...] = jnp.zeros_like(ext1)
    ext2[...] = jnp.zeros_like(ext2)
    barrier, count = greet()
    for peer in across + along:
        pl.semaphore_signal(barrier, inc=1, device_id=peer, device_id_type=MESH)

    def split_columns(ext, lowest, columns, rows, depth):
        def step(index, carry):
            x = index // columns + lowest
            y = index % columns + lowest
            values = [ext[x, y, z] for z in depth]
            parts = []
            for value in values:
                high = value.astype(BF).astype(F32)
                parts.append(jnp.concatenate([high, value - high, jnp.zeros((8, 128), F32)], axis=0).astype(BF))
            for z, made in zip(depth, parts):
                halves[(x * ey_size + y) * ez_size + z] = made
            return carry

        lax.fori_loop(0, columns * rows, step, 0)

    def tile_sum(x, y, z, offsets):
        total = None
        for dx, dy, dz in offsets:
            slot = ((x * ny + y) * nz + z) * 27 + (dx + 1) * 9 + (dy + 1) * 3 + dz + 1
            e = ((x + 1 + dx) * ey_size + y + 1 + dy) * ez_size + z + 1 + dz
            both = jnp.concatenate([store[slot, 0], store[slot, 1]], axis=1)
            out = jnp.dot(halves[e], both, preferred_element_type=F32)
            total = out if total is None else total + out
        return total[:8]

    columns = [(x, y) for x in range(nx) for y in range(ny)]

    def inside(x, y):
        return [(dx, dy) for dx in INSIDE[x] for dy in INSIDE[y]]

    def outside(x, y):
        return [d for d in FLAT if d not in inside(x, y)]

    def level_pass():
        def step(index, carry):
            for sub in range(2):
                z = index * 2 + sub
                for x, y in columns:
                    acc[(x * ny + y) * nz + z] = tile_sum(x, y, z, [d + (0,) for d in inside(x, y)])
            return carry

        lax.fori_loop(0, nz // 2, step, 0)

    def between_pass():
        def step(z, carry):
            for x, y in columns:
                t = (x * ny + y) * nz + z
                acc[t] = acc[t] + tile_sum(x, y, z, [d + (1,) for d in inside(x, y)])
                acc[t + 1] = acc[t + 1] + tile_sum(x, y, z + 1, [d + (-1,) for d in inside(x, y)])
            return carry

        lax.fori_loop(0, nz - 1, step, 0)

    def rim_pass():
        for x, y in columns:
            for z, dz in ((0, -1), (nz - 1, 1)):
                t = (x * ny + y) * nz + z
                acc[t] = acc[t] + tile_sum(x, y, z, [d + (dz,) for d in inside(x, y)])

        def step(index, carry):
            for sub in range(2):
                z = index * 2 + sub
                for x, y in columns:
                    t = (x * ny + y) * nz + z
                    around = [d + (dz,) for d in outside(x, y) for dz in (-1, 0, 1)]
                    acc[t] = acc[t] + tile_sum(x, y, z, around)
            return carry

        lax.fori_loop(0, nz // 2, step, 0)

    def finish(vector, image, following):
        def step(index, carry):
            x = index // ny
            y = index % ny
            made = []
            for z in range(nz):
                t = index * nz + z
                value = vector[x, y, z]
                out = image_rows(acc[t], diagonal[t], coupling[index, z : z + 1, :], value)
                made.append((out, out - SHIFT * value))
            for z, (out, rest) in enumerate(made):
                image[index * nz + z] = out
                if following is not None:
                    following[x, y, z] = rest
            return carry

        lax.fori_loop(0, nx * ny, step, 0)

    own_depth = range(1, nz + 1)
    whole = range(nz + 2)
    ext1[1:-1, 1:-1, 1:-1] = u1[...]
    split_columns(ext1, 1, ny, nx, own_depth)
    level_pass()
    pl.semaphore_wait(barrier, count + (len(across) + len(along)))
    send_rims(((u1, ext1),), rim_send.at[pl.ds(0, 1)], rim_recv.at[pl.ds(0, 1)])
    between_pass()
    await_rims(((u1, ext1),), rim_send.at[pl.ds(0, 1)], rim_recv.at[pl.ds(0, 1)])
    split_columns(ext1, 0, ny + 2, nx + 2, whole)
    rim_pass()
    finish(u1, w1, u2)

    ext2[1:-1, 1:-1, 1:-1] = u2[...]
    split_columns(ext2, 1, ny, nx, own_depth)
    send_rims(((u2, ext2),), rim_send.at[pl.ds(1, 1)], rim_recv.at[pl.ds(1, 1)])
    level_pass()
    between_pass()
    await_rims(((u2, ext2),), rim_send.at[pl.ds(1, 1)], rim_recv.at[pl.ds(1, 1)])
    split_columns(ext2, 0, ny + 2, nx + 2, whole)
    rim_pass()
    finish(u2, w2, None)

    owned = nx * ny * nz
    tile = (owned, 4, 128)
    b0, b1, b2 = (u[...].reshape(tile) for u in (u0, u1, u2))
    a0, a1, a2 = (w[...].reshape(tile) for w in (w0, w1, w2))
    wanted = [(b0, b0), (b0, b1), (b0, b2), (b0, a0), (b0, a1), (b0, a2), (b1, a1), (b1, a2), (b2, a2)]
    sums = []
    for left, right in wanted:
        both = jnp.sum(left * right, axis=0)
        sums.append(both[0:2] + both[2:4])
    stacked = jnp.concatenate(sums + [jnp.zeros((128 - 18, 128), F32)], axis=0)
    part[0] = jnp.sum(stacked.T, axis=0, keepdims=True)

    def gather(turn, peers, here, stage, width):
        made = []
        for index, peer in enumerate(peers):
            copy = pltpu.make_async_remote_copy(
                part.at[turn],
                stage.at[here],
                send_sem.at[turn, index],
                recv_sem.at[turn, index],
                device_id=peer,
                device_id_type=MESH,
            )
            copy.start()
            made.append(copy)
        stage[here] = part[turn]
        for copy in made:
            copy.wait_recv()
        total = jnp.sum(stage[...], axis=0)
        for copy in made:
            copy.wait_send()
        return total

    part[1] = gather(0, across, gy * sizes[2] + gz, plane, len(across) + 1)
    total = gather(1, along, gx, line, len(along) + 1)
    m0, m1, m2, g00, g01, g02, g11, g12, g22 = (total[:, 2 * k : 2 * k + 2] for k in range(9))
    f1 = g01 / g00
    f2 = g02 / g00
    h11 = g11 - f1 * g01
    h12 = g12 - f1 * g02
    h22 = g22 - f2 * g02
    n1 = m1 - f1 * m0
    n2 = m2 - f2 * m0
    f3 = h12 / h11
    k22 = h22 - f3 * h12
    k2 = n2 - f3 * n1
    c2 = k2 / k22
    c1 = (n1 - h12 * c2) / h11
    c0 = (m0 - g01 * c1 - g02 * c2) / g00

    def spread(c):
        pair = [jnp.broadcast_to(c[:, r : r + 1], (1, 128)) for r in range(2)]
        return jnp.concatenate(pair + pair, axis=0)[None]

    c0, c1, c2 = (spread(c) for c in (c0, c1, c2))
    answer = c0 * b0 + c1 * b1 + c2 * b2
    left = b0 - (c0 * a0 + c1 * a1 + c2 * a2)
    for t in range(32):
        for f in range(4):
            solution[f, t // 8, t % 8 : t % 8 + 1, :] = answer[t, f : f + 1]
            residual[f, t // 8, t % 8 : t % 8 + 1, :] = left[t, f : f + 1]


def on_device(positions, shield, width, hardness, softness, coupling, pair_bits, right_side):
    nx, ny, nz, lanes = hardness.shape
    owned = nx * ny * nz
    ext = (nx + 2, ny + 2, nz + 2)
    tiles = ext[0] * ext[1] * ext[2]

    def kept(value):
        return pltpu.with_memory_space_constraint(value, pltpu.VMEM)

    def far(value):
        return pltpu.with_memory_space_constraint(value, pltpu.HBM)

    def limits(size, **more):
        return pltpu.CompilerParams(vmem_limit_bytes=size, **more)

    slots = owned * 27 + 3
    param_ext, field_ext, blank = pl.pallas_call(
        first_halo,
        out_shape=(
            pltpu.VMEM(ext + (8, lanes), F32),
            pltpu.VMEM(ext + (1, lanes), F32),
            pltpu.VMEM((slots - slots % 5, 2, lanes, lanes), BF),
        ),
        in_specs=[pl.BlockSpec(memory_space=pltpu.HBM)] * 4,
        out_specs=(VMEM_SPEC,) * 3,
        scratch_shapes=[
            pltpu.VMEM((nx, ny, nz, 8, lanes), F32),
            pltpu.VMEM((nx, ny, nz, 1, lanes), F32),
            pltpu.VMEM((lanes, lanes), F32),
            pltpu.VMEM(positions.shape, F32),
            pltpu.VMEM(shield.shape, F32),
            pltpu.VMEM(width.shape, F32),
            pltpu.VMEM(right_side.shape, F32),
            pltpu.SemaphoreType.DMA((4,)),
            pltpu.SemaphoreType.DMA((2, 26)),
            pltpu.SemaphoreType.DMA((2, 26)),
        ],
        compiler_params=limits(LIMIT, collective_id=0, has_side_effects=True),
        name="first_halo",
    )(*(far(a) for a in (positions, shield, width, right_side)))

    hard, soft, link = (a.reshape(owned // 8, 8, lanes) for a in (hardness, softness, coupling))
    store, diagonal, image0, own0, own1 = pl.pallas_call(
        build,
        out_shape=(pltpu.VMEM(blank.shape, BF),) + (pltpu.VMEM((owned, 4, lanes), F32),) * 4,
        in_specs=[SMEM_SPEC] + [VMEM_SPEC] * 6,
        input_output_aliases={6: 0},
        out_specs=(VMEM_SPEC,) * 5,
        scratch_shapes=[
            pltpu.VMEM((tiles, lanes, lanes), BF),
            pltpu.VMEM((owned, 48, 2 * lanes), BF),
            pltpu.VMEM((tiles, 16, lanes), BF),
            pltpu.VMEM((owned + 1, 16, 2 * lanes), F32),
            pltpu.SMEM((owned * 27 + GROUP,), jnp.int32),
            pltpu.VMEM((GROUP, 2, lanes, lanes), BF),
        ],
        compiler_params=limits(LIMIT),
        name="build",
    )(
        pair_bits,
        kept(param_ext.reshape(tiles, 8, lanes)),
        kept(field_ext.reshape(tiles, 1, lanes)),
        hard,
        soft,
        link,
        kept(blank),
    )

    line = lax.axis_size("gx")
    plane = lax.axis_size("gy") * lax.axis_size("gz")
    shape = pltpu.VMEM((4, owned // 8, 8, lanes), F32)
    answer, left = pl.pallas_call(
        solve,
        out_shape=(shape, shape),
        in_specs=[VMEM_SPEC] * 8,
        out_specs=(VMEM_SPEC, VMEM_SPEC),
        scratch_shapes=[
            pltpu.VMEM(ext + (4, lanes), F32),
            pltpu.VMEM(ext + (4, lanes), F32),
            pltpu.VMEM((nx, ny, nz, 4, lanes), F32),
            pltpu.VMEM((owned, 4, lanes), F32),
            pltpu.VMEM((owned, 4, lanes), F32),
            pltpu.VMEM((tiles, 16, lanes), BF),
            pltpu.VMEM((owned, 8, 2 * lanes), F32),
            pltpu.VMEM((2, 1, lanes), F32),
            pltpu.VMEM((plane, 1, lanes), F32),
            pltpu.VMEM((line, 1, lanes), F32),
            pltpu.SemaphoreType.DMA((2, 26)),
            pltpu.SemaphoreType.DMA((2, 26)),
            pltpu.SemaphoreType.DMA((2, plane - 1)),
            pltpu.SemaphoreType.DMA((2, plane - 1)),
        ],
        compiler_params=limits(LIMIT, collective_id=1, has_side_effects=True),
        name="solve",
    )(kept(own0), kept(own1.reshape(nx, ny, nz, 4, lanes)), kept(image0), kept(diagonal), link, kept(store),
      kept(param_ext.reshape(tiles, 8, lanes)), kept(field_ext.reshape(tiles, 1, lanes)))
    out = (4, nx, ny, nz, lanes)
    return answer.reshape(out), left.reshape(out)


def solution(mesh):
    tile = P("gx", "gy", "gz", None)
    field = P(None, "gx", "gy", "gz", None)
    return jax.shard_map(
        on_device,
        mesh=mesh,
        in_specs=(field, tile, tile, tile, tile, tile, P("gx", "gy", "gz"), field),
        out_specs=(field, field),
        check_vma=False,
    )
```
